32 devices in a mesh: rep: 2 (over x), dp: 16 (over y, z, core).
Axes of the slice: x: 2, y: 2, z: 4, core: 2. Of those that a mesh axis runs over, the one named last changes fastest.
Arguments:
- x: bfloat16 [32, 1024, 512], P(('rep', 'dp')), parts along dimension 0
- dy: bfloat16 [32, 1024, 512], P(('rep', 'dp')), parts along dimension 0
- w_gate: bfloat16 [2, 512, 8192], P(None, 'dp')
- w_up: bfloat16 [2, 512, 8192], P(None, 'dp')
- w_down: bfloat16 [2, 8192, 512], P(None, 'dp')
Outputs:
- output 1: bfloat16 [32, 1024, 512], P(('rep', 'dp')), parts along dimension 0
- output 2: bfloat16 [4, 512, 8192], P('rep', 'dp'), parts along dimension 0
- output 3: bfloat16 [4, 512, 8192], P('rep', 'dp'), parts along dimension 0
- output 4: bfloat16 [4, 8192, 512], P('rep', 'dp'), parts along dimension 0
There are 2 independent parts. The reference program is written for one: setup_inputs(seed, part) draws one part's arguments, and reference() takes and returns one part's arrays. A program takes and returns all parts, laid end to end along the dimension named above; an argument that names none is the same for every part.
All inputs are finite; a program needn't handle non-finite values.
Results may differ from the reference program's by a relative error of at most 0.018.
Values are sent between devices in bfloat16 or wider.
A program may use at most 2 GiB of HBM per device.

```python
import jax
import jax.numpy as jnp
from jax import lax

SEQUENCES = 16
TOKENS = 1024
D = 512
FF = 8192
LAYERS = 2
NAMES = ("w_gate", "w_up", "w_down")
SHAPES = {"w_gate": (LAYERS, D, FF), "w_up": (LAYERS, D, FF), "w_down": (LAYERS, FF, D)}


def bump(key, n, height):
    away = (jnp.arange(n, dtype=jnp.int32) - jax.random.randint(key, (), 0, n, jnp.int32)) % n
    return jnp.where(away < n // 8, height, 1.0)


def together(key, own, strength):
    shared = jax.random.normal(key, own.shape[1:], jnp.float32)
    return (own + strength * shared) * lax.rsqrt(1 + strength * strength)


def setup_inputs(seed: int = 0, part: int = 0) -> dict:
    kx, kdy, ka, kb, kz, kf, kh, kl, *kw = jax.random.split(jax.random.key(seed), 8 + len(NAMES))
    kx, kdy, ka, kb = (jax.random.fold_in(k, part) for k in (kx, kdy, ka, kb))
    shape = (SEQUENCES, TOKENS, D)
    much_x, much_dy = jax.random.uniform(kz, (2,), jnp.float32, 0.0, 1.0)
    layers = 2.0 ** jax.random.uniform(kl, (LAYERS, 1, 1), jnp.float32, -1.0, 1.0)
    x = together(ka, jax.random.normal(kx, shape, jnp.float32), much_x) * bump(kf, D, 4.0)
    dy = together(kb, jax.random.normal(kdy, shape, jnp.float32), much_dy)
    drawn = {"x": x.astype(jnp.bfloat16), "dy": (dy * (SEQUENCES * TOKENS) ** -0.5).astype(jnp.bfloat16)}
    for key, name in zip(kw, NAMES, strict=True):
        w = jax.random.normal(key, SHAPES[name], jnp.float32) * SHAPES[name][1] ** -0.5
        drawn[name] = (w * {"w_gate": 1.0, "w_up": bump(kh, FF, 4.0), "w_down": layers}[name]).astype(jnp.bfloat16)
    return drawn


def matmul(a, w):
    return jnp.dot(a, w, preferred_element_type=jnp.float32).astype(jnp.bfloat16)


def normed(h):
    wide = h.astype(jnp.float32)
    scale = lax.rsqrt(jnp.mean(wide**2, -1, keepdims=True) + 1e-6)
    return (wide * scale).astype(jnp.bfloat16)


def layer(h, w):
    a = normed(h)
    gate = jnp.dot(a, w["w_gate"], preferred_element_type=jnp.float32)
    up = jnp.dot(a, w["w_up"], preferred_element_type=jnp.float32)
    return h + matmul((jax.nn.silu(gate) * up).astype(jnp.bfloat16), w["w_down"])


def stack(weights, h):
    return lax.scan(lambda h, w: (layer(h, w), None), h, weights)[0]


def reference(x, dy, w_gate, w_up, w_down):
    weights = dict(zip(NAMES, (w_gate, w_up, w_down), strict=True))

    def take(so_far, sequence):
        h, by_y = sequence
        _, back = jax.vjp(stack, weights, h)
        by_weights, by_h = back(by_y)
        return jax.tree.map(lambda total, term: total + term.astype(jnp.float32), so_far, by_weights), by_h

    none_yet = {name: jnp.zeros(w.shape, jnp.float32) for name, w in weights.items()}
    by_weights, by_x = lax.scan(take, none_yet, (x, dy))
    return (by_x, *(by_weights[name].astype(jnp.bfloat16) for name in NAMES))
```

```python
import functools

import jax
import jax.numpy as jnp
from jax import lax
from jax.experimental import pallas as pl
from jax.experimental.pallas import tpu as pltpu
from jax.sharding import PartitionSpec as P

MESH = pl.DeviceIdType.MESH
F32, BF16 = jnp.float32, jnp.bfloat16
ROUNDS = 12
ALL = 2 * ROUNDS
T_SLOTS, R_SLOTS, S_SLOTS = 8, 6, 8


def nn(a, b):
    return jnp.dot(a, b, preferred_element_type=F32)


def nt(a, b):
    return lax.dot_general(a, b, (((1,), (1,)), ((), ())), preferred_element_type=F32)


def kernel(tile, x_ref, dy_ref, wgu_ref, wd_ref, dx_ref, og_ref, od_ref, xp_ref, h1_ref,
           W, T, R, A, AT, DY, DYT, ACC, PT, ACT, DG, DU,
           prep_loc, prep_send, prep_rem, ag_send, ag_recv, ax_send, ax_recv,
           rs_send, rs_recv, out_loc, out_send, out_recv, ex_send, ex_recv, loc, credit):
    tok, d = x_ref.shape
    half = wd_ref.shape[3]
    rows = half // 2
    rep, dp = lax.axis_index("rep"), lax.axis_index("dp")
    core, chip = lax.rem(dp, 2), dp // 2
    q = jnp.where(chip < 4, chip, 11 - chip)

    def chip_at(place):
        place = lax.rem(place + 16, 8)
        return jnp.where(place < 4, place, 11 - place)

    ring = tuple((rep, 2 * chip_at(q + step) + core) for step in (1, -1))
    across, mate = (1 - rep, dp), (rep, 2 * chip + 1 - core)

    def remote(src, dst, send, recv, to):
        return pltpu.make_async_remote_copy(
            src_ref=src, dst_ref=dst, send_sem=send, recv_sem=recv, device_id=to, device_id_type=MESH
        )

    barrier = pltpu.get_barrier_semaphore()
    for other in (*ring, across, mate):
        pl.semaphore_signal(barrier, inc=1, device_id=other, device_id_type=MESH)

    mine, theirs = pl.ds(core * tok, tok), pl.ds((1 - core) * tok, tok)
    own_rows = pl.ds(pl.multiple_of(core * rows, rows), rows)
    mate_rows = pl.ds(pl.multiple_of((1 - core) * rows, rows), rows)

    def prep_down(r):
        return pltpu.make_async_copy(wd_ref.at[r // ROUNDS, lax.rem(r, ROUNDS) // 3], W.at[r, chip], prep_loc.at[r])

    def up_index(r):
        return lax.rem(r, ROUNDS) // 3, jnp.maximum(lax.rem(r, 3) - 1, 0)

    def prep_here(r):
        dst = W.at[r, chip, :, own_rows]
        return pltpu.make_async_copy(wgu_ref.at[(r // ROUNDS, core, *up_index(r))], dst, prep_loc.at[r])

    def prep_there(r):
        src, dst = wgu_ref.at[(r // ROUNDS, 1 - core, *up_index(r))], W.at[r, chip, :, own_rows]
        return remote(src, dst, prep_send.at[r], prep_rem.at[r], mate)

    def start_local(r, _):
        @pl.when(lax.rem(r, 3) == 0)
        def _():
            prep_down(r).start()

        @pl.when(lax.rem(r, 3) != 0)
        def _():
            prep_here(r).start()

        return 0

    lax.fori_loop(0, ALL, start_local, 0)
    load_x = pltpu.make_async_copy(x_ref, A.at[mine], loc.at[0])
    load_dy = pltpu.make_async_copy(dy_ref, DY.at[mine], loc.at[1])
    load_x.start()
    load_dy.start()
    pl.semaphore_wait(barrier, 4)

    def start_mate(r, _):
        @pl.when(lax.rem(r, 3) != 0)
        def _():
            prep_there(r).start()

        return 0

    send_x = remote(x_ref, A.at[mine], ex_send.at[0], ex_recv.at[0], mate)
    send_xp = remote(x_ref, xp_ref, ex_send.at[1], ex_recv.at[1], mate)
    send_dy = remote(dy_ref, DY.at[mine], ex_send.at[2], ex_recv.at[2], mate)
    lax.fori_loop(0, 3, start_mate, 0)
    send_x.start()
    lax.fori_loop(3, ALL, start_mate, 0)
    send_xp.start()
    send_dy.start()

    def wait_prep(r):
        @pl.when(lax.rem(r, 3) == 0)
        def _():
            prep_down(r).wait()

        @pl.when(lax.rem(r, 3) != 0)
        def _():
            prep_here(r).wait()
            prep_there(r).wait_recv()

    def kind(r):
        return lax.rem(r, 3)

    def hops(r, way):
        return 4 - lax.rem(r + way + 8, 2)

    def gathers(r):
        return (kind(r) == 2) | (kind(r) == rep)

    def ag_copy(r, way, h):
        piece = W.at[r, chip_at(q - h if way == 0 else q + h)]
        return remote(piece, piece, ag_send.at[lax.rem(r, S_SLOTS), way, h], ag_recv.at[r, way, h], ring[way])

    def ag_retire(r):
        for way in (0, 1):
            for h in range(4):
                @pl.when(gathers(r) & (h < hops(r, way)))
                def _():
                    ag_copy(r, way, h).wait_send()

    def ag_event(n, h):
        r = n - h
        ok = (r >= 0) & (r < ALL)

        @pl.when(ok & (h == 0))
        def _():
            wait_prep(r)

            @pl.when(r >= S_SLOTS)
            def _():
                ag_retire(r - S_SLOTS)

        @pl.when(ok & gathers(jnp.maximum(r, 0)))
        def _():
            for way in (0, 1):
                @pl.when(h == 0)
                def _():
                    ag_copy(r, way, 0).start()

                @pl.when((h > 0) & (h <= hops(r, way)))
                def _():
                    piece = W.at[r, chip_at(q - h if way == 0 else q + h)]
                    remote(piece, piece, ag_send.at[0, way, 0], ag_recv.at[r, way, h - 1], ring[way]).wait_recv()

                    @pl.when(h < hops(r, way))
                    def _():
                        ag_copy(r, way, h).start()

                    @pl.when(kind(r) != 2)
                    def _():
                        remote(piece, piece, ax_send.at[r], ax_recv.at[r], across).start()

    def ag_ready(r):
        @pl.when(jnp.logical_not(gathers(r)))
        def _():
            seven = W.at[r, pl.ds(0, 7)]
            remote(seven, seven, ax_send.at[r], ax_recv.at[r], across).wait_recv()

    def ag_events(lo, hi):
        def body(e, _):
            ag_event(e // 5, 4 - lax.rem(e, 5))
            return 0

        lax.fori_loop(lo, hi, body, 0)

    def rs_copy(n, way, h):
        slot = lax.rem(n, T_SLOTS)
        step = hops(n, way) - h
        return remote(
            T.at[slot, chip_at(q + step if way == 0 else q - step)],
            R.at[lax.rem(n, R_SLOTS), 4 * way + h],
            rs_send.at[slot, way, h],
            rs_recv.at[lax.rem(n, R_SLOTS), way, h],
            ring[way],
        )

    def out_down(n):
        slot = lax.rem(n, T_SLOTS)
        return pltpu.make_async_copy(
            T.at[slot, chip], od_ref.at[1 - n // ROUNDS, lax.rem(n, ROUNDS) // 3], out_loc.at[slot]
        )

    def out_up(n):
        return og_ref.at[1 - n // ROUNDS, core, lax.rem(n, ROUNDS) // 3, jnp.minimum(lax.rem(n, 3), 1)]

    def out_here(n):
        slot = lax.rem(n, T_SLOTS)
        return pltpu.make_async_copy(T.at[slot, chip, :, own_rows], out_up(n), out_loc.at[slot])

    def out_there(n):
        slot = lax.rem(n, T_SLOTS)
        return remote(T.at[slot, chip, :, mate_rows], out_up(n), out_send.at[slot], out_recv.at[n], mate)

    def rs_retire(n):
        for way in (0, 1):
            for h in range(4):
                @pl.when(h < hops(n, way))
                def _():
                    rs_copy(n, way, h).wait_send()

        @pl.when(kind(n) == 2)
        def _():
            out_down(n).wait()

        @pl.when(kind(n) != 2)
        def _():
            out_here(n).wait()
            out_there(n).wait_send()

    def rs_event(n0, h):
        n = n0 - h
        ok = (n >= 0) & (n < ALL)

        @pl.when(ok)
        def _():
            slot, rslot = lax.rem(n, T_SLOTS), lax.rem(n, R_SLOTS)
            for way in (0, 1):
                @pl.when(h == 0)
                def _():
                    @pl.when(n >= R_SLOTS)
                    def _():
                        pl.semaphore_wait(credit.at[way], 1)

                    rs_copy(n, way, 0).start()

                @pl.when((h > 0) & (h <= hops(n, way)))
                def _():
                    rs_copy(n, way, h - 1).wait_recv()

                    @pl.when(h < hops(n, way))
                    def _():
                        step = hops(n, way) - h
                        own = chip_at(q + step if way == 0 else q - step)
                        total = T[slot, own].astype(F32) + R[rslot, 4 * way + h - 1].astype(F32)
                        T[slot, own] = total.astype(BF16)
                        rs_copy(n, way, h).start()

            @pl.when(h == 4)
            def _():
                total = T[slot, chip].astype(F32) + R[rslot, hops(n, 0) - 1].astype(F32)
                total = total + R[rslot, 4 + hops(n, 1) - 1].astype(F32)
                T[slot, chip] = total.astype(BF16)

                @pl.when(kind(n) == 2)
                def _():
                    out_down(n).start()

                @pl.when(kind(n) != 2)
                def _():
                    out_here(n).start()
                    out_there(n).start()

                @pl.when(n < ALL - R_SLOTS)
                def _():
                    for way in (0, 1):
                        pl.semaphore_signal(credit.at[way], inc=1, device_id=ring[1 - way], device_id_type=MESH)

    def rs_events(lo, hi):
        def body(e, _):
            rs_event(e // 5, 4 - lax.rem(e, 5))
            return 0

        lax.fori_loop(lo, hi, body, 0)

    block = min(256, tok)
    blocks = 2 * tok // block

    def part(t, size=block):
        return pl.ds(pl.multiple_of(t * size, size), size)

    def normed(h):
        wide = h.astype(F32)
        return (wide * lax.rsqrt(jnp.mean(wide * wide, -1, keepdims=True) + 1e-6)).astype(BF16)

    def norm_all(flip):
        def body(t, _):
            a = normed(A[part(t), :])
            A[part(t), :] = a
            if flip:
                AT[:, part(t)] = a.T
            return 0

        lax.fori_loop(0, blocks, body, 0)

    def flip_dy():
        def body(t, _):
            DYT[:, part(t)] = DY[part(t), :].T
            return 0

        lax.fori_loop(0, blocks, body, 0)

    def clear():
        def body(t, _):
            ACC[part(t), :] = jnp.zeros((block, d), F32)
            return 0

        lax.fori_loop(0, blocks, body, 0)

    def own_block(t):
        return pl.ds(pl.multiple_of(core * tok + t * block, block), block)

    def forward(j):
        i, hh = j // 2, lax.rem(j, 2)
        r = 3 * i + 1 + hh

        def body(t, _):
            at = A[part(t, tile), :]
            gate = nn(at, W[r, :, 0].reshape(d, -1))
            up = nn(at, W[r, :, 1].reshape(d, -1))
            act = (gate * (0.5 * jnp.tanh(0.5 * gate) + 0.5) * up).astype(BF16)
            ACC[part(t, tile), :] += nn(act, W[3 * i, pl.ds(4 * hh, 4)].reshape(-1, d))
            return 0

        lax.fori_loop(0, 2 * tok // tile, body, 0)

    def first(n, _):
        @pl.when(n == 1)
        def _():
            load_x.wait()
            send_x.wait_recv()
            norm_all(False)
            clear()

        @pl.when(n == 3)
        def _():
            load_dy.wait()
            send_dy.wait_recv()
            flip_dy()

        pair = (n - 4) // 3

        @pl.when((n >= 4) & (lax.rem(n, 3) == 0))
        def _():
            ag_ready(3 * pair)
            ag_ready(3 * pair + 1)
            forward(2 * pair)

        ag_events(5 * n, 5 * n + 5)

        @pl.when((n >= 4) & (lax.rem(n, 3) == 0))
        def _():
            ag_ready(3 * pair + 2)
            forward(2 * pair + 1)

        return 0

    lax.fori_loop(0, 16, first, 0)

    swap = remote(ACC.at[theirs], PT, ex_send.at[3], ex_recv.at[3], mate)
    swap.start()
    fetch = pltpu.make_async_copy(x_ref, DG.at[pl.ds(0, tok)], loc.at[2])
    fetch.start()
    ag_events(80, 85)
    fetch.wait()
    swap.wait()

    def residual(t, _):
        mlp = (ACC[own_block(t), :] + PT[part(t), :]).astype(BF16)
        h = (DG[part(t), :].astype(F32) + mlp.astype(F32)).astype(BF16)
        ACT[part(t), :] = h
        A[own_block(t), :] = h
        return 0

    lax.fori_loop(0, tok // block, residual, 0)
    h1 = ACT.at[pl.ds(0, tok)]
    send_h = remote(h1, A.at[mine], ex_send.at[4], ex_recv.at[4], mate)
    keep_h = pltpu.make_async_copy(h1, h1_ref, loc.at[3])
    send_h.start()
    keep_h.start()
    clear()
    ag_events(85, 90)
    send_h.wait()
    keep_h.wait()
    norm_all(True)

    def norm_back(h_ref, t):
        by_a = (ACC[own_block(t), :] + PT[part(t), :]).astype(BF16).astype(F32)
        wide = h_ref[part(t), :].astype(F32)
        scale = lax.rsqrt(jnp.mean(wide * wide, -1, keepdims=True) + 1e-6)
        along = jnp.mean(by_a * wide, -1, keepdims=True)
        by_h = (by_a * scale - wide * (scale * scale * scale * along)).astype(BF16)
        return (DY[own_block(t), :].astype(F32) + by_h.astype(F32)).astype(BF16)

    def chunk(c, _):
        l = 1 - c // 8
        j = lax.rem(c, 8)
        i, hh = j // 2, lax.rem(j, 2)
        pair = c // 2
        base = ROUNDS * l + 3 * i
        up_slot, down_slot = lax.rem(3 * pair + hh, T_SLOTS), lax.rem(3 * pair + 2, T_SLOTS)

        def serve(slot):
            ag_lo, ag_hi = 90 + 10 * c + (10 * slot) // 8, 90 + 10 * c + (10 * slot + 10) // 8
            ag_events(jnp.minimum(ag_lo, 140), jnp.minimum(ag_hi, 140))
            odd = lax.rem(c, 2) == 1
            count = jnp.where(odd | (c == 8), 5, 10)
            start = jnp.where(odd, 15 * pair, 15 * pair - count)
            lo, hi = start + (count * slot) // 8, start + (count * slot + count) // 8
            rs_events(jnp.maximum(lo, 0), jnp.maximum(hi, 0))

        @pl.when(c == 8)
        def _():
            swap = remote(ACC.at[theirs], PT, ex_send.at[5], ex_recv.at[5], mate)
            swap.start()
            fetch = pltpu.make_async_copy(h1_ref, DG.at[pl.ds(0, tok)], loc.at[4])
            fetch.start()
            rs_events(50, 53)
            fetch.wait()
            swap.wait()

            def body(t, _):
                dh = norm_back(DG, t)
                DY[own_block(t), :] = dh
                ACT[part(t), :] = dh
                return 0

            lax.fori_loop(0, tok // block, body, 0)
            send = remote(ACT.at[pl.ds(0, tok)], DY.at[mine], ex_send.at[6], ex_recv.at[6], mate)
            send.start()
            again = pltpu.make_async_copy(x_ref, A.at[mine], loc.at[5])
            again.start()
            send_xp.wait_recv()
            other = pltpu.make_async_copy(xp_ref, A.at[theirs], loc.at[6])
            other.start()
            clear()
            rs_events(53, 55)
            again.wait()
            other.wait()
            norm_all(True)
            send.wait()
            flip_dy()

        @pl.when(l == 1)
        def _():
            @pl.when(hh == 0)
            def _():
                ag_ready(base)

            ag_ready(base + 1 + hh)

        def tokens(t, _):
            s = part(t, tile)
            at = A[s, :]
            wg, wu = W[base + 1 + hh, :, 0].reshape(d, -1), W[base + 1 + hh, :, 1].reshape(d, -1)
            gate, up = nn(at, wg), nn(at, wu)
            by_act = nt(DY[s, :], W[base, pl.ds(4 * hh, 4)].reshape(-1, d)).astype(BF16).astype(F32)
            sig = 0.5 * jnp.tanh(0.5 * gate) + 0.5
            silu = gate * sig
            ACT[s, :] = (silu * up).astype(BF16)
            dup = (by_act * silu).astype(BF16)
            dgate = (by_act * up * (sig + silu * (1.0 - sig))).astype(BF16)
            DG[s, :] = dgate
            DU[s, :] = dup
            ACC[s, :] += nt(dgate, wg) + nt(dup, wu)
            serve(t * (4 * tile) // (2 * tok))
            return 0

        lax.fori_loop(0, 2 * tok // tile, tokens, 0)

        for back, when in ((0, 0), (1, 1), (2, 0)):
            n = 3 * pair + back - T_SLOTS

            @pl.when((hh == when) & (n >= 0))
            def _():
                rs_retire(n)

        def grads_up(p, _):
            s = pl.ds(pl.multiple_of(p * (d // 2), d // 2), d // 2)
            T[up_slot, pl.ds(4 * p, 4), 0] = nn(AT[s, :], DG[...]).astype(BF16).reshape(4, half, -1)
            T[up_slot, pl.ds(4 * p, 4), 1] = nn(AT[s, :], DU[...]).astype(BF16).reshape(4, half, -1)
            serve(4 + p)
            return 0

        lax.fori_loop(0, 2, grads_up, 0)

        for p in range(2):
            s = slice(p * (d // 2), (p + 1) * (d // 2))
            g = nn(DYT[s, :], ACT[...]).T.astype(BF16)
            T[down_slot, pl.ds(4 * hh, 4), :, :, s] = g.reshape(4, 2, half, d // 2)
            serve(6 + p)

        return 0

    lax.fori_loop(0, 16, chunk, 0)

    swap = remote(ACC.at[theirs], PT, ex_send.at[7], ex_recv.at[7], mate)
    swap.start()
    fetch = pltpu.make_async_copy(x_ref, DG.at[pl.ds(0, tok)], loc.at[7])
    fetch.start()
    rs_events(110, 115)
    fetch.wait()
    swap.wait()

    def last(t, _):
        ACT[part(t), :] = norm_back(DG, t)
        return 0

    lax.fori_loop(0, tok // block, last, 0)
    put = pltpu.make_async_copy(ACT.at[pl.ds(0, tok)], dx_ref, loc.at[8])
    put.start()
    rs_events(115, 140)

    put.wait()
    for copy in (send_x, send_xp, send_dy):
        copy.wait_send()

    def sent(r, _):
        @pl.when(lax.rem(r, 3) != 0)
        def _():
            prep_there(r).wait_send()

        @pl.when((kind(r) != 2) & (kind(r) == rep))
        def _():
            seven = W.at[r, pl.ds(0, 7)]
            remote(seven, seven, ax_send.at[r], ax_recv.at[r], across).wait_send()

        @pl.when(r >= ALL - S_SLOTS)
        def _():
            ag_retire(r)

        @pl.when(r >= ALL - T_SLOTS)
        def _():
            rs_retire(r)

        @pl.when(kind(r) != 2)
        def _():
            out_there(r).wait_recv()

        return 0

    lax.fori_loop(0, ALL, sent, 0)


def of_a_device(x, dy, w_gate, w_up, w_down):
    _, tok, d = x.shape
    layers, rows, ff = w_gate.shape
    half = 2 * rows
    strip = ff // 64
    wgu = jnp.stack((w_gate, w_up)).reshape(2, layers, rows, 2, 4, 2, 4, strip)
    wgu = wgu.transpose(1, 5, 6, 3, 0, 2, 4, 7).reshape(layers, 2, 4, 2, 2, rows, 4 * strip)
    wd = w_down.reshape(layers, 4, 2, half, d)
    hbm = pl.BlockSpec(memory_space=pltpu.HBM)
    tile = tok // 2
    piece = (2, half, d)
    both = 2 * tok
    dx, og, od, _, _ = pl.pallas_call(
        functools.partial(kernel, tile),
        out_shape=(
            jax.ShapeDtypeStruct((tok, d), BF16),
            jax.ShapeDtypeStruct(wgu.shape, BF16),
            jax.ShapeDtypeStruct(wd.shape, BF16),
            jax.ShapeDtypeStruct((tok, d), BF16),
            jax.ShapeDtypeStruct((tok, d), BF16),
        ),
        in_specs=[hbm] * 4,
        out_specs=[hbm] * 5,
        scratch_shapes=[
            pltpu.VMEM((ALL, 8, *piece), BF16),
            pltpu.VMEM((T_SLOTS, 8, *piece), BF16),
            pltpu.VMEM((R_SLOTS, 8, *piece), BF16),
            pltpu.VMEM((both, d), BF16),
            pltpu.VMEM((d, both), BF16),
            pltpu.VMEM((both, d), BF16),
            pltpu.VMEM((d, both), BF16),
            pltpu.VMEM((both, d), F32),
            pltpu.VMEM((tok, d), F32),
            pltpu.VMEM((both, 4 * strip), BF16),
            pltpu.VMEM((both, 4 * strip), BF16),
            pltpu.VMEM((both, 4 * strip), BF16),
            pltpu.SemaphoreType.DMA((ALL,)),
            pltpu.SemaphoreType.DMA((ALL,)),
            pltpu.SemaphoreType.DMA((ALL,)),
            pltpu.SemaphoreType.DMA((S_SLOTS, 2, 4)),
            pltpu.SemaphoreType.DMA((ALL, 2, 4)),
            pltpu.SemaphoreType.DMA((ALL,)),
            pltpu.SemaphoreType.DMA((ALL,)),
            pltpu.SemaphoreType.DMA((T_SLOTS, 2, 4)),
            pltpu.SemaphoreType.DMA((R_SLOTS, 2, 4)),
            pltpu.SemaphoreType.DMA((T_SLOTS,)),
            pltpu.SemaphoreType.DMA((T_SLOTS,)),
            pltpu.SemaphoreType.DMA((ALL,)),
            pltpu.SemaphoreType.DMA((8,)),
            pltpu.SemaphoreType.DMA((8,)),
            pltpu.SemaphoreType.DMA((9,)),
            pltpu.SemaphoreType.REGULAR((2,)),
        ],
        compiler_params=pltpu.CompilerParams(
            collective_id=0, has_side_effects=True, vmem_limit_bytes=67043328
        ),
    )(x[0], dy[0], wgu, wd)
    og = og.reshape(layers, 2, 4, 2, 2, rows, 4, strip)
    og = og.transpose(4, 0, 5, 3, 6, 1, 2, 7).reshape(2, layers, rows, ff)
    return dx[None], og[0], og[1], od.reshape(layers, 4 * 2 * half, d)


def solution(mesh):
    by_seq, by_row = P(("rep", "dp"), None, None), P(None, "dp", None)
    out = P("rep", "dp", None)
    return jax.shard_map(
        of_a_device,
        mesh=mesh,
        in_specs=(by_seq, by_seq, by_row, by_row, by_row),
        out_specs=(by_seq, out, out, out),
        check_vma=False,
    )
```

```python
import functools

import jax
import jax.numpy as jnp
from jax import lax
from jax.experimental import pallas as pl
from jax.experimental.pallas import tpu as pltpu
from jax.sharding import PartitionSpec as P

MESH = pl.DeviceIdType.MESH
F32, BF16 = jnp.float32, jnp.bfloat16
ROUNDS = 12
ALL = 2 * ROUNDS
T_SLOTS, R_SLOTS, S_SLOTS = 8, 6, 8
BETWEEN = 48, 54


def events_by(c):
    return jnp.where(c <= 8, jnp.maximum((13 * c - 8) // 2, 0), (15 * c - 11) // 2)


def nn(a, b):
    return jnp.dot(a, b, preferred_element_type=F32)


def nt(a, b):
    return lax.dot_general(a, b, (((1,), (1,)), ((), ())), preferred_element_type=F32)


def kernel(tile, x_ref, dy_ref, wg_ref, wu_ref, wd_ref, dx_ref, og_ref, od_ref, xp_ref, h1_ref,
           W, R, A, AT, DY, DYT, ACC, PT, ACT, DG, DU,
           prep_loc, prep_up, prep_send, prep_rem, ag_send, ag_recv, ax_send, ax_recv,
           rs_send, rs_recv, out_loc, out_send, out_recv, ex_send, ex_recv, sw_send, sw_recv, loc, credit):
    tok, d = x_ref.shape
    half = wd_ref.shape[3]
    rows = half // 2
    strip = wg_ref.shape[2] // 64
    assert d == 4 * strip and half == strip // 2
    rep, dp = lax.axis_index("rep"), lax.axis_index("dp")
    core, chip = lax.rem(dp, 2), dp // 2
    q = jnp.where(chip < 4, chip, 11 - chip)

    def chip_at(place):
        place = lax.rem(place + 16, 8)
        return jnp.where(place < 4, place, 11 - place)

    ring = tuple((rep, 2 * chip_at(q + step) + core) for step in (1, -1))
    across, mate = (1 - rep, dp), (rep, 2 * chip + 1 - core)

    def remote(src, dst, send, recv, to):
        return pltpu.make_async_remote_copy(
            src_ref=src, dst_ref=dst, send_sem=send, recv_sem=recv, device_id=to, device_id_type=MESH
        )

    barrier = pltpu.get_barrier_semaphore()
    for other in (*ring, across, mate):
        pl.semaphore_signal(barrier, inc=1, device_id=other, device_id_type=MESH)

    mine, theirs = pl.ds(core * tok, tok), pl.ds((1 - core) * tok, tok)
    own_rows = pl.ds(pl.multiple_of(core * rows, rows), rows)
    mate_rows = pl.ds(pl.multiple_of((1 - core) * rows, rows), rows)

    def kind(r):
        return lax.rem(r, 3)

    def prep_down(r):
        src = wd_ref.at[r // ROUNDS, lax.rem(r, ROUNDS) // 3]
        return pltpu.make_async_copy(src, W.at[r, chip], prep_loc.at[r // 3])

    def staged(l, g, b, columns=slice(None)):
        spot = 16 * g + b
        return 8 * l + spot // 4, lax.rem(spot // 2, 2), pl.ds(pl.multiple_of(rows * lax.rem(spot, 2), rows), rows), columns

    def load_up(l):
        def body(b, _):
            for g, ref in enumerate((wg_ref, wu_ref)):
                src = ref.at[l, :, pl.ds(pl.multiple_of(d * b, d), d)]
                pltpu.make_async_copy(src, R.at[staged(l, g, b)], prep_up.at[l]).start()
            return 0

        lax.fori_loop(0, 16, body, 0)

    def loaded_up(l):
        eight = R.at[pl.ds(8 * l, 8)]
        pltpu.make_async_copy(eight, eight, prep_up.at[l]).wait()

    def up_number(r):
        return 2 * (r // 3) + kind(r) - 1

    def mate_part(r, g):
        return pl.ds(pl.multiple_of((2 * up_number(r) + g) * rows, rows), rows)

    def prep_start(r):
        l, i, hh = r // ROUNDS, lax.rem(r, ROUNDS) // 3, kind(r) - 1
        columns = pl.ds(pl.multiple_of(strip * i, strip), strip)
        for g in range(2):
            for s in range(4):
                place = slice(strip * s, strip * (s + 1))
                b = 2 * (4 * hh + s)
                W[r, chip, g, own_rows, place] = R[staged(l, g, b + core, columns)]
                DG[mate_part(r, g), place] = R[staged(l, g, b + 1 - core, columns)]
            dst = W.at[r, chip, g, own_rows]
            remote(DG.at[mate_part(r, g)], dst, prep_send, prep_rem.at[up_number(r)], mate).start()

    def prep_there(r):
        part = W.at[r, chip, :, own_rows]
        return remote(part, part, prep_send, prep_rem.at[up_number(r)], mate)

    def prep_first(r, _):
        prep_down(3 * r).start()
        return 0

    load_up(0)
    lax.fori_loop(0, ALL // 3, prep_first, 0)
    load_up(1)

    def prep_all(lo, hi):
        def body(r, _):
            @pl.when(kind(r) != 0)
            def _():
                prep_start(r)

            return 0

        lax.fori_loop(lo, hi, body, 0)

    load_x = pltpu.make_async_copy(x_ref, A.at[mine], loc.at[0])
    load_dy = pltpu.make_async_copy(dy_ref, DY.at[mine], loc.at[1])
    load_x.start()
    load_dy.start()
    pl.semaphore_wait(barrier, 4)

    send_x = remote(x_ref, A.at[mine], ex_send.at[0], ex_recv.at[0], mate)
    send_xp = remote(x_ref, xp_ref, ex_send.at[1], ex_recv.at[1], mate)
    send_dy = remote(dy_ref, DY.at[mine], ex_send.at[2], ex_recv.at[2], mate)
    loaded_up(0)
    prep_all(0, 3)
    send_x.start()
    send_xp.start()
    send_dy.start()

    def wait_prep(r):
        @pl.when(lax.rem(r, 3) == 0)
        def _():
            prep_down(r).wait()

        @pl.when(lax.rem(r, 3) != 0)
        def _():
            prep_there(r).wait_recv()

    def hops(r, way):
        return 4 - lax.rem(r + way + 8, 2)

    def shared(r):
        return (r >= ROUNDS) | (kind(r) != 2)

    def gathers(r):
        first = (kind(r) == 2) | (kind(r) == rep)
        return jnp.where(r < ROUNDS, first, lax.rem(r, 2) == rep)

    def ag_copy(r, way, h):
        piece = W.at[r, chip_at(q - h if way == 0 else q + h)]
        return remote(piece, piece, ag_send.at[lax.rem(r, S_SLOTS), way], ag_recv.at[lax.rem(r, S_SLOTS), way, h], ring[way])

    def ag_retire(r):
        for way in (0, 1):
            for count in (3, 4):
                @pl.when(gathers(r) & (hops(r, way) == count))
                def _():
                    sent = W.at[r, pl.ds(0, count)]
                    remote(sent, sent, ag_send.at[lax.rem(r, S_SLOTS), way], ag_recv.at[0, way, 0], ring[way]).wait_send()

    def ag_event(n, h):
        r = n - h
        ok = (r >= 0) & (r < ALL)

        @pl.when(ok & (h == 0))
        def _():
            wait_prep(r)

            @pl.when(r >= S_SLOTS)
            def _():
                ag_retire(r - S_SLOTS)

        @pl.when(ok & gathers(jnp.maximum(r, 0)))
        def _():
            for way in (0, 1):
                @pl.when(h == 0)
                def _():
                    ag_copy(r, way, 0).start()

                @pl.when((h > 0) & (h <= hops(r, way)))
                def _():
                    piece = W.at[r, chip_at(q - h if way == 0 else q + h)]
                    ag_copy(r, way, h - 1).wait_recv()

                    @pl.when(h < hops(r, way))
                    def _():
                        ag_copy(r, way, h).start()

                    @pl.when(shared(r))
                    def _():
                        remote(piece, piece, ax_send.at[r // ROUNDS], ax_recv.at[r], across).start()

    def ag_ready(r):
        @pl.when(jnp.logical_not(gathers(r)))
        def _():
            seven = W.at[r, pl.ds(0, 7)]
            remote(seven, seven, ax_send.at[0], ax_recv.at[r], across).wait_recv()

    def across_sent(l):
        some = W.at[pl.ds(0, 7), pl.ds(0, 4)] if l == 0 else W.at[pl.ds(0, 7), pl.ds(0, 6)]
        remote(some, some, ax_send.at[l], ax_recv.at[0], across).wait_send()

    def ag_events(lo, hi):
        def body(e, _):
            ag_event(e // 5, 4 - lax.rem(e, 5))
            return 0

        lax.fori_loop(lo, hi, body, 0)

    def term(n):
        return jnp.where(n < ROUNDS, ALL + lax.rem(n, T_SLOTS), n)

    def own_sem(n):
        return lax.rem(n, T_SLOTS)

    def came(n, way, h):
        return 7 * lax.rem(n, R_SLOTS) + (h if way == 0 else hops(n, 0) + h)

    def rs_copy(n, way, h):
        slot = own_sem(n)
        step = hops(n, way) - h
        return remote(
            W.at[term(n), chip_at(q + step if way == 0 else q - step)],
            R.at[came(n, way, h)],
            rs_send.at[slot, way],
            rs_recv.at[lax.rem(n, R_SLOTS), way, h],
            ring[way],
        )

    def out_down(n):
        return pltpu.make_async_copy(
            W.at[term(n), chip], od_ref.at[1 - n // ROUNDS, lax.rem(n, ROUNDS) // 3], out_loc.at[own_sem(n)]
        )

    def out_up(n):
        return og_ref.at[1 - n // ROUNDS, core, lax.rem(n, ROUNDS) // 3, jnp.minimum(kind(n), 1)]

    def out_here(n):
        return pltpu.make_async_copy(W.at[term(n), chip, :, own_rows], out_up(n), out_loc.at[own_sem(n)])

    def out_there(n):
        part = W.at[term(n), chip, :, mate_rows]
        number = 2 * (n // 3) + jnp.minimum(kind(n), 1)
        return remote(part, out_up(n), out_send.at[own_sem(n)], out_recv.at[number], mate)

    def rs_retire(n):
        for way in (0, 1):
            for count in (3, 4):
                @pl.when(hops(n, way) == count)
                def _():
                    sent = W.at[term(n), pl.ds(0, count)]
                    remote(sent, sent, rs_send.at[own_sem(n), way], rs_recv.at[0, way, 0], ring[way]).wait_send()

        @pl.when(kind(n) == 2)
        def _():
            out_down(n).wait()

        @pl.when(kind(n) != 2)
        def _():
            out_here(n).wait()
            out_there(n).wait_send()

    def rs_event(n0, h):
        n = n0 - h
        ok = (n >= 0) & (n < ALL)

        @pl.when(ok)
        def _():
            slot = term(n)
            for way in (0, 1):
                @pl.when(h == 0)
                def _():
                    @pl.when(n >= R_SLOTS)
                    def _():
                        pl.semaphore_wait(credit.at[way], 1)

                    rs_copy(n, way, 0).start()

                @pl.when((h > 0) & (h <= hops(n, way)))
                def _():
                    rs_copy(n, way, h - 1).wait_recv()

                    @pl.when(h < hops(n, way))
                    def _():
                        step = hops(n, way) - h
                        own = chip_at(q + step if way == 0 else q - step)
                        total = W[slot, own].astype(F32) + R[came(n, way, h - 1)].astype(F32)
                        W[slot, own] = total.astype(BF16)
                        rs_copy(n, way, h).start()

            @pl.when(h == 4)
            def _():
                total = W[slot, chip].astype(F32) + R[came(n, 0, hops(n, 0) - 1)].astype(F32)
                total = total + R[came(n, 1, hops(n, 1) - 1)].astype(F32)
                W[slot, chip] = total.astype(BF16)

                @pl.when(kind(n) == 2)
                def _():
                    out_down(n).start()

                @pl.when(kind(n) != 2)
                def _():
                    out_here(n).start()
                    out_there(n).start()

                @pl.when(n < ALL - R_SLOTS)
                def _():
                    for way in (0, 1):
                        pl.semaphore_signal(credit.at[way], inc=1, device_id=ring[1 - way], device_id_type=MESH)

    def rs_events(lo, hi):
        def body(e, _):
            rs_event(e // 5, 4 - lax.rem(e, 5))
            return 0

        lax.fori_loop(lo, hi, body, 0)

    block = min(256, tok)
    blocks = 2 * tok // block

    def part(t, size=block):
        return pl.ds(pl.multiple_of(t * size, size), size)

    def normed(h):
        wide = h.astype(F32)
        return (wide * lax.rsqrt(jnp.mean(wide * wide, -1, keepdims=True) + 1e-6)).astype(BF16)

    def norm_block(c, flip):
        def body(t, _):
            s = pl.ds(pl.multiple_of(c * tok + t * block, block), block)
            a = normed(A[s, :])
            A[s, :] = a
            if flip:
                AT[:, s] = a.T
            return 0

        lax.fori_loop(0, tok // block, body, 0)

    def flip_dy(c):
        def body(t, _):
            s = pl.ds(pl.multiple_of(c * tok + t * block, block), block)
            DYT[:, s] = DY[s, :].T
            return 0

        lax.fori_loop(0, tok // block, body, 0)

    def clear():
        def body(t, _):
            ACC[part(t), :] = jnp.zeros((block, d), F32)
            return 0

        lax.fori_loop(0, blocks, body, 0)

    def own_block(t):
        return pl.ds(pl.multiple_of(core * tok + t * block, block), block)

    def nth(t):
        return part(lax.rem(t + 2 * (1 - core), 4), tile)

    def swap(k, t):
        src = ACC.at[pl.ds(pl.multiple_of((1 - core) * tok + t * tile, tile), tile)]
        return remote(src, PT.at[part(t, tile)], sw_send.at[k, t], sw_recv.at[k, t], mate)

    def forward(j, after):
        i, hh = j // 2, lax.rem(j, 2)
        r = 3 * i + 1 + hh

        def body(t, _):
            s = nth(t)
            at = A[s, :]
            gate = nn(at, W[r, :, 0].reshape(d, -1))
            up = nn(at, W[r, :, 1].reshape(d, -1))
            act = (gate * (0.5 * jnp.tanh(0.5 * gate) + 0.5) * up).astype(BF16)
            ACC[s, :] += nn(act, W[3 * i, pl.ds(4 * hh, 4)].reshape(-1, d))

            @pl.when((j == 7) & (t < 2))
            def _():
                swap(0, t).start()

            after(t)
            return 0

        lax.fori_loop(0, 4, body, 0)

    ag_events(0, 5)
    prep_all(3, ROUNDS)
    loaded_up(1)
    prep_all(ROUNDS, ALL)
    load_x.wait()
    norm_block(core, False)
    ag_events(5, 9)
    send_x.wait_recv()
    norm_block(1 - core, False)
    clear()
    ag_events(9, 15)
    load_dy.wait()
    flip_dy(core)
    ag_events(15, 20)
    send_dy.wait_recv()
    flip_dy(1 - core)
    ag_events(20, 27)

    def first(j, _):
        i, hh = j // 2, lax.rem(j, 2)

        @pl.when(hh == 0)
        def _():
            ag_ready(3 * i)

        ag_ready(3 * i + 1 + hh)
        lo = 27 + (15 * j) // 2
        count = 27 + (15 * (j + 1)) // 2 - lo
        forward(j, lambda t: ag_events(lo + (count * t) // 4, lo + (count * (t + 1)) // 4))
        return 0

    lax.fori_loop(0, 8, first, 0)

    whole = DG.at[pl.ds(0, 4 * ALL // 3 * rows)]
    remote(whole, whole, prep_send, prep_rem.at[0], mate).wait_send()
    fetch = pltpu.make_async_copy(x_ref, DG.at[pl.ds(0, tok)], loc.at[2])
    fetch.start()
    ag_events(87, 90)
    fetch.wait()
    swap(0, 0).wait()
    swap(0, 1).wait()

    def residual(t, _):
        mlp = (ACC[own_block(t), :] + PT[part(t), :]).astype(BF16)
        h = (DG[part(t), :].astype(F32) + mlp.astype(F32)).astype(BF16)
        ACT[part(t), :] = h
        A[own_block(t), :] = h
        return 0

    lax.fori_loop(0, tok // block, residual, 0)
    h1 = ACT.at[pl.ds(0, tok)]
    send_h = remote(h1, A.at[mine], ex_send.at[3], ex_recv.at[3], mate)
    keep_h = pltpu.make_async_copy(h1, h1_ref, loc.at[3])
    send_h.start()
    keep_h.start()
    clear()
    norm_block(core, True)
    ag_events(90, 95)
    send_h.wait()
    norm_block(1 - core, True)
    ag_events(95, 100)
    keep_h.wait()

    def norm_back(h_ref, t):
        by_a = (ACC[own_block(t), :] + PT[part(t), :]).astype(BF16).astype(F32)
        wide = h_ref[part(t), :].astype(F32)
        scale = lax.rsqrt(jnp.mean(wide * wide, -1, keepdims=True) + 1e-6)
        along = jnp.mean(by_a * wide, -1, keepdims=True)
        by_h = (by_a * scale - wide * (scale * scale * scale * along)).astype(BF16)
        return (DY[own_block(t), :].astype(F32) + by_h.astype(F32)).astype(BF16)

    def chunk(c, _):
        l = 1 - c // 8
        j = lax.rem(c, 8)
        i, hh = j // 2, lax.rem(j, 2)
        pair = c // 2
        base = ROUNDS * l + 3 * i
        up_slot, down_slot = term(3 * pair + hh), term(3 * pair + 2)

        lo = jnp.where(c == 8, BETWEEN[1], events_by(c))
        count = events_by(c + 1) - lo

        def serve(slot):
            ag_lo, ag_hi = 100 + 10 * c + (10 * slot) // 8, 100 + 10 * c + (10 * slot + 10) // 8
            ag_events(jnp.minimum(ag_lo, 140), jnp.minimum(ag_hi, 140))
            rs_events(lo + (count * slot) // 8, lo + (count * slot + count) // 8)

        @pl.when(c == 8)
        def _():
            start, end = BETWEEN
            again = pltpu.make_async_copy(x_ref, A.at[mine], loc.at[5])
            again.start()
            send_xp.wait_recv()
            other = pltpu.make_async_copy(xp_ref, A.at[theirs], loc.at[6])
            other.start()
            fetch = pltpu.make_async_copy(h1_ref, DG.at[pl.ds(0, tok)], loc.at[4])
            fetch.start()
            rs_events(start, start + 1)
            fetch.wait()
            swap(1, 0).wait()
            swap(1, 1).wait()

            def body(t, _):
                dh = norm_back(DG, t)
                DY[own_block(t), :] = dh
                ACT[part(t), :] = dh
                return 0

            lax.fori_loop(0, tok // block, body, 0)
            send = remote(ACT.at[pl.ds(0, tok)], DY.at[mine], ex_send.at[4], ex_recv.at[4], mate)
            send.start()
            clear()
            flip_dy(core)
            rs_events(start + 1, start + 2)
            again.wait()
            norm_block(core, True)
            rs_events(start + 2, start + 3)
            other.wait()
            norm_block(1 - core, True)
            rs_events(start + 3, end)
            send.wait()
            flip_dy(1 - core)

            def gone(r, _):
                ag_retire(r)
                return 0

            lax.fori_loop(ALL - S_SLOTS, ALL, gone, 0)
            across_sent(1)

        @pl.when(l == 1)
        def _():
            @pl.when(hh == 0)
            def _():
                ag_ready(base)

            ag_ready(base + 1 + hh)

        def tokens(t, _):
            s = nth(t)
            at = A[s, :]
            wg, wu = W[base + 1 + hh, :, 0].reshape(d, -1), W[base + 1 + hh, :, 1].reshape(d, -1)
            gate, up = nn(at, wg), nn(at, wu)
            by_act = nt(DY[s, :], W[base, pl.ds(4 * hh, 4)].reshape(-1, d)).astype(BF16).astype(F32)
            sig = 0.5 * jnp.tanh(0.5 * gate) + 0.5
            silu = gate * sig
            ACT[s, :] = (silu * up).astype(BF16)
            dup = (by_act * silu).astype(BF16)
            dgate = (by_act * up * (sig + silu * (1.0 - sig))).astype(BF16)
            DG[s, :] = dgate
            DU[s, :] = dup
            ACC[s, :] += nt(dgate, wg) + nt(dup, wu)

            @pl.when((j == 7) & (t < 2))
            def _():
                swap(2 - l, t).start()

            serve(t)
            return 0

        lax.fori_loop(0, 4, tokens, 0)

        for back, when in ((0, 0), (1, 1), (2, 0)):
            n = 3 * pair + back - T_SLOTS

            @pl.when((hh == when) & (n >= 0))
            def _():
                rs_retire(n)

        def grads_up(p, _):
            s = pl.ds(pl.multiple_of(p * (d // 2), d // 2), d // 2)
            W[up_slot, pl.ds(4 * p, 4), 0] = nn(AT[s, :], DG[...]).astype(BF16).reshape(4, half, -1)
            W[up_slot, pl.ds(4 * p, 4), 1] = nn(AT[s, :], DU[...]).astype(BF16).reshape(4, half, -1)
            serve(4 + p)
            return 0

        lax.fori_loop(0, 2, grads_up, 0)

        for p in range(2):
            s = slice(p * (d // 2), (p + 1) * (d // 2))
            g = nn(DYT[s, :], ACT[...]).T.astype(BF16)
            W[down_slot, pl.ds(4 * hh, 4), :, :, s] = g.reshape(4, 2, half, d // 2)
            serve(6 + p)

        return 0

    lax.fori_loop(0, 16, chunk, 0)

    fetch = pltpu.make_async_copy(x_ref, DG.at[pl.ds(0, tok)], loc.at[7])
    fetch.start()
    rs_events(114, 115)
    fetch.wait()
    swap(2, 0).wait()
    swap(2, 1).wait()

    def last(t, _):
        ACT[part(t), :] = norm_back(DG, t)
        return 0

    lax.fori_loop(0, tok // block, last, 0)
    put = pltpu.make_async_copy(ACT.at[pl.ds(0, tok)], dx_ref, loc.at[8])
    put.start()
    rs_events(115, 140)

    put.wait()
    for copy in (send_x, send_xp, send_dy):
        copy.wait_send()

    def sent(r, _):
        @pl.when(r >= ALL - T_SLOTS)
        def _():
            rs_retire(r)

        @pl.when(kind(r) != 2)
        def _():
            out_there(r).wait_recv()

        return 0

    across_sent(0)
    lax.fori_loop(0, ALL, sent, 0)


def put_kernel(dx_ref, og_ref, od_ref, dx_out, dwg_out, dwu_out, dwd_out, dx, og, od, dwg, dwu, came, went):
    layers = dwg.shape[0]
    strip = dwg.shape[2] // 64
    loads = [pltpu.make_async_copy(og_ref.at[l], og.at[l], came.at[l]) for l in range(layers)]
    others = [(dx_ref, dx, dx_out), (od_ref, od, dwd_out)]
    for copy in loads:
        copy.start()
    for k, (src, buffer, _) in enumerate(others):
        pltpu.make_async_copy(src, buffer, came.at[2 + k]).start()
    for l in range(layers):
        loads[l].wait()
        for part in range(16):
            c, i, hh = part // 8, part // 2 % 4, part % 2
            for s in range(4):
                column = strip * (8 * (4 * hh + s) + 4 * c + i)
                for g, out in enumerate((dwg, dwu)):
                    out[l, :, column : column + strip] = og[l, c, i, hh, g, :, strip * s : strip * (s + 1)]
        pltpu.make_async_copy(dwg.at[l], dwg_out.at[l], went.at[2 * l]).start()
        pltpu.make_async_copy(dwu.at[l], dwu_out.at[l], went.at[2 * l + 1]).start()
    for k, (src, buffer, dst) in enumerate(others):
        pltpu.make_async_copy(src, buffer, came.at[2 + k]).wait()
        pltpu.make_async_copy(buffer, dst, went.at[4 + k]).start()
    for l in range(layers):
        pltpu.make_async_copy(dwg.at[l], dwg_out.at[l], went.at[2 * l]).wait()
        pltpu.make_async_copy(dwu.at[l], dwu_out.at[l], went.at[2 * l + 1]).wait()
    for k, (_, buffer, dst) in enumerate(others):
        pltpu.make_async_copy(buffer, dst, went.at[4 + k]).wait()


def of_a_device(x, dy, w_gate, w_up, w_down):
    _, tok, d = x.shape
    layers, rows, ff = w_gate.shape
    half = 2 * rows
    strip = ff // 64
    wd = w_down.reshape(layers, 4, 2, half, d)
    hbm = pl.BlockSpec(memory_space=pltpu.HBM)
    tile = tok // 2
    piece = (2, half, d)
    both = 2 * tok
    dma = pltpu.SemaphoreType.DMA
    up = (layers, 2, 4, 2, 2, rows, 4 * strip)
    dx, og, od, _, _ = pl.pallas_call(
        functools.partial(kernel, tile),
        out_shape=tuple(
            jax.ShapeDtypeStruct(shape, BF16)
            for shape in ((tok, d), up, wd.shape, (tok, d), (tok, d))
        ),
        in_specs=[hbm] * 5,
        out_specs=[hbm] * 5,
        scratch_shapes=[
            pltpu.VMEM((ALL + T_SLOTS, 8, *piece), BF16),
            pltpu.VMEM((7 * R_SLOTS, *piece), BF16),
            pltpu.VMEM((both, d), BF16),
            pltpu.VMEM((d, both), BF16),
            pltpu.VMEM((both, d), BF16),
            pltpu.VMEM((d, both), BF16),
            pltpu.VMEM((both, d), F32),
            pltpu.VMEM((tok, d), F32),
            pltpu.VMEM((both, 4 * strip), BF16),
            pltpu.VMEM((both, 4 * strip), BF16),
            pltpu.VMEM((both, 4 * strip), BF16),
            dma((ALL // 3,)),
            dma((layers,)),
            dma(()),
            dma((2 * ALL // 3,)),
            dma((S_SLOTS, 2)),
            dma((S_SLOTS, 2, 4)),
            dma((2,)),
            dma((ALL,)),
            dma((T_SLOTS, 2)),
            dma((R_SLOTS, 2, 4)),
            dma((T_SLOTS,)),
            dma((T_SLOTS,)),
            dma((2 * ALL // 3,)),
            dma((5,)),
            dma((5,)),
            dma((3, 2)),
            dma((3, 2)),
            dma((9,)),
            pltpu.SemaphoreType.REGULAR((2,)),
        ],
        compiler_params=pltpu.CompilerParams(
            collective_id=0, has_side_effects=True, vmem_limit_bytes=67043328
        ),
    )(x[0], dy[0], w_gate, w_up, wd)
    results = (dx.shape, w_gate.shape, w_up.shape, od.shape)
    dx, dwg, dwu, dwd = pl.pallas_call(
        put_kernel,
        out_shape=tuple(jax.ShapeDtypeStruct(shape, BF16) for shape in results),
        in_specs=[hbm] * 3,
        out_specs=[hbm] * 4,
        scratch_shapes=[
            *(pltpu.VMEM(shape, BF16) for shape in (dx.shape, up, od.shape, w_gate.shape, w_up.shape)),
            dma((4,)),
            dma((6,)),
        ],
    )(dx, og, od)
    return dx[None], dwg, dwu, dwd.reshape(w_down.shape)


def solution(mesh):
    by_seq, by_row = P(("rep", "dp"), None, None), P(None, "dp", None)
    out = P("rep", "dp", None)
    return jax.shard_map(
        of_a_device,
        mesh=mesh,
        in_specs=(by_seq, by_seq, by_row, by_row, by_row),
        out_specs=(by_seq, out, out, out),
        check_vma=False,
    )
```

```python
import functools

import jax
import jax.numpy as jnp
from jax import lax
from jax.experimental import pallas as pl
from jax.experimental.pallas import tpu as pltpu
from jax.sharding import PartitionSpec as P

MESH = pl.DeviceIdType.MESH
F32, BF16 = jnp.float32, jnp.bfloat16
ROUNDS = 12
ALL = 2 * ROUNDS
T_SLOTS, R_SLOTS, S_SLOTS = 8, 6, 8
GATHERED = 14
FIRST = (21, 27, 31, 37, 41, 47, 50, 52, 55)
BETWEEN = 44, 50
LAST_AG, LAST_RS = 5 * (GATHERED - 1) + 17, 5 * (ALL - 1) + 17


def events_by(c):
    return jnp.where(c <= 8, jnp.maximum((13 * c - 16) // 2, 0), (15 * c - 19) // 2)


def pick(values, k):
    out = values[-1]
    for number, value in enumerate(values[:-1]):
        out = jnp.where(k == number, value, out)
    return out


def nn(a, b):
    return jnp.dot(a, b, preferred_element_type=F32)


def nt(a, b):
    return lax.dot_general(a, b, (((1,), (1,)), ((), ())), preferred_element_type=F32)


def kernel(tile, x_ref, dy_ref, wg_ref, wu_ref, wd_ref, dx_ref, og_ref, od_ref, xp_ref, h1_ref,
           W, R, A, AT, DY, DYT, ACC, PT, ACT, DG, DU,
           prep_loc, prep_up, prep_send, prep_rem, ag_send, ag_recv, ax_send, ax_recv,
           rs_send, rs_recv, out_loc, out_send, out_recv, ex_send, ex_recv, sw_send, sw_recv, loc, credit):
    tok, d = x_ref.shape
    half = wd_ref.shape[3]
    rows = half // 2
    strip = wg_ref.shape[2] // 64
    assert d == 4 * strip and half == strip // 2
    rep, dp = lax.axis_index("rep"), lax.axis_index("dp")
    core, chip = lax.rem(dp, 2), dp // 2
    q = jnp.where(chip < 4, chip, 11 - chip)

    def chip_at(place):
        place = lax.rem(place + 16, 8)
        return jnp.where(place < 4, place, 11 - place)

    ring = tuple((rep, 2 * chip_at(q + step) + core) for step in (1, -1))
    across, mate = (1 - rep, dp), (rep, 2 * chip + 1 - core)

    def remote(src, dst, send, recv, to):
        return pltpu.make_async_remote_copy(
            src_ref=src, dst_ref=dst, send_sem=send, recv_sem=recv, device_id=to, device_id_type=MESH
        )

    barrier = pltpu.get_barrier_semaphore()
    for other in (*ring, across, mate):
        pl.semaphore_signal(barrier, inc=1, device_id=other, device_id_type=MESH)

    mine, theirs = pl.ds(core * tok, tok), pl.ds((1 - core) * tok, tok)
    own_rows = pl.ds(pl.multiple_of(core * rows, rows), rows)
    mate_rows = pl.ds(pl.multiple_of((1 - core) * rows, rows), rows)

    def kind(r):
        return lax.rem(r, 3)

    def prep_down(r):
        src = wd_ref.at[r // ROUNDS, lax.rem(r, ROUNDS) // 3]
        return pltpu.make_async_copy(src, W.at[r, chip], prep_loc.at[r // 3])

    def staged(l, g, b, columns=slice(None)):
        spot = 16 * g + b
        return 8 * l + spot // 4, lax.rem(spot // 2, 2), pl.ds(pl.multiple_of(rows * lax.rem(spot, 2), rows), rows), columns

    def load_up(l):
        def body(b, _):
            for g, ref in enumerate((wg_ref, wu_ref)):
                src = ref.at[l, :, pl.ds(pl.multiple_of(d * b, d), d)]
                pltpu.make_async_copy(src, R.at[staged(l, g, b)], prep_up.at[l]).start()
            return 0

        lax.fori_loop(0, 16, body, 0)

    def loaded_up(l):
        eight = R.at[pl.ds(8 * l, 8)]
        pltpu.make_async_copy(eight, eight, prep_up.at[l]).wait()

    def up_number(r):
        return 2 * (r // 3) + kind(r) - 1

    def mate_part(r, g):
        return pl.ds(pl.multiple_of((2 * up_number(r) + g) * rows, rows), rows)

    def prep_start(r):
        l, i, hh = r // ROUNDS, lax.rem(r, ROUNDS) // 3, kind(r) - 1
        columns = pl.ds(pl.multiple_of(strip * i, strip), strip)
        for g in range(2):
            for s in range(4):
                place = slice(strip * s, strip * (s + 1))
                b = 2 * (4 * hh + s)
                W[r, chip, g, own_rows, place] = R[staged(l, g, b + core, columns)]
                DG[mate_part(r, g), place] = R[staged(l, g, b + 1 - core, columns)]
            dst = W.at[r, chip, g, own_rows]
            remote(DG.at[mate_part(r, g)], dst, prep_send, prep_rem.at[up_number(r)], mate).start()

    def prep_there(r):
        part = W.at[r, chip, :, own_rows]
        return remote(part, part, prep_send, prep_rem.at[up_number(r)], mate)

    def prep_first(r, _):
        prep_down(3 * r).start()
        return 0

    load_up(0)
    lax.fori_loop(0, ALL // 3, prep_first, 0)
    load_up(1)

    def prep_all(lo, hi):
        def body(r, _):
            @pl.when(kind(r) != 0)
            def _():
                prep_start(r)

            return 0

        lax.fori_loop(lo, hi, body, 0)

    load_x = pltpu.make_async_copy(x_ref, A.at[mine], loc.at[0])
    load_dy = pltpu.make_async_copy(dy_ref, DY.at[mine], loc.at[1])
    load_x.start()
    load_dy.start()
    pl.semaphore_wait(barrier, 4)

    send_x = remote(x_ref, A.at[mine], ex_send.at[0], ex_recv.at[0], mate)
    send_xp = remote(x_ref, xp_ref, ex_send.at[1], ex_recv.at[1], mate)
    send_dy = remote(dy_ref, DY.at[mine], ex_send.at[2], ex_recv.at[2], mate)
    loaded_up(0)
    prep_all(0, 3)
    send_x.start()
    send_xp.start()
    send_dy.start()

    def wait_prep(r):
        @pl.when(lax.rem(r, 3) == 0)
        def _():
            prep_down(r).wait()

        @pl.when(lax.rem(r, 3) != 0)
        def _():
            prep_there(r).wait_recv()

    def hops(r, way):
        return 4 - lax.rem(r + way + 8, 2)

    def shared(r):
        return (r >= ROUNDS) | (kind(r) != 2)

    def gathers(r):
        first = (kind(r) == 2) | (kind(r) == rep)
        return jnp.where(r < ROUNDS, first, (r - ROUNDS) // 6 == rep)

    def gathered(g):
        return jnp.where(
            g < 8, pick((rep, 3 + rep, 2, 6 + rep, 5, 9 + rep, 8, 11), g), ROUNDS + 6 * rep + g - 8
        )

    def ag_copy(g, r, way, h):
        piece = W.at[r, chip_at(q - h if way == 0 else q + h)]
        slot = lax.rem(g, S_SLOTS)
        return remote(piece, piece, ag_send.at[slot, way], ag_recv.at[slot, way, h], ring[way])

    def ag_retire(g):
        for way in (0, 1):
            for count in (3, 4):
                @pl.when(hops(g, way) == count)
                def _():
                    sent = W.at[0, pl.ds(0, count)]
                    remote(sent, sent, ag_send.at[lax.rem(g, S_SLOTS), way], ag_recv.at[0, way, 0], ring[way]).wait_send()

    def ag_event(g, h):
        @pl.when((g >= 0) & (g < GATHERED))
        def _():
            r = gathered(g)

            @pl.when(h == 0)
            def _():
                wait_prep(r)

                @pl.when(g >= S_SLOTS)
                def _():
                    ag_retire(g - S_SLOTS)

            for way in (0, 1):
                @pl.when(h == 0)
                def _():
                    ag_copy(g, r, way, 0).start()

                @pl.when((h > 0) & (h <= hops(g, way)))
                def _():
                    ag_copy(g, r, way, h - 1).wait_recv()

                    @pl.when(h < hops(g, way))
                    def _():
                        ag_copy(g, r, way, h).start()

                    @pl.when(shared(r))
                    def _():
                        piece = W.at[r, chip_at(q - h if way == 0 else q + h)]
                        remote(piece, piece, ax_send.at[r // ROUNDS], ax_recv.at[r], across).start()

    def ag_ready(r):
        @pl.when(jnp.logical_not(gathers(r)))
        def _():
            wait_prep(r)
            seven = W.at[r, pl.ds(0, 7)]
            remote(seven, seven, ax_send.at[0], ax_recv.at[r], across).wait_recv()

    def across_sent(l):
        some = W.at[pl.ds(0, 7), pl.ds(0, 4)] if l == 0 else W.at[pl.ds(0, 7), pl.ds(0, 6)]
        remote(some, some, ax_send.at[l], ax_recv.at[0], across).wait_send()

    def ag_events(lo, hi):
        def body(e, _):
            h = lax.rem(4 * e, 5)
            ag_event((e - 4 * h) // 5, h)
            return 0

        lax.fori_loop(lo, hi, body, 0)

    def turn(l, k):
        return jnp.where(l == 1, lax.rem(k + 2 * rep, 4), k)

    def strip_of(n):
        return turn(1 - n // ROUNDS, lax.rem(n, ROUNDS) // 3)

    def term(n):
        return jnp.where(n < ROUNDS, ALL + lax.rem(n, T_SLOTS), n)

    def own_sem(n):
        return lax.rem(n, T_SLOTS)

    def came(n, way, h):
        return 7 * lax.rem(n, R_SLOTS) + (h if way == 0 else hops(n, 0) + h)

    def rs_copy(n, way, h):
        slot = own_sem(n)
        step = hops(n, way) - h
        return remote(
            W.at[term(n), chip_at(q + step if way == 0 else q - step)],
            R.at[came(n, way, h)],
            rs_send.at[slot, way],
            rs_recv.at[lax.rem(n, R_SLOTS), way, h],
            ring[way],
        )

    def out_down(n):
        return pltpu.make_async_copy(
            W.at[term(n), chip], od_ref.at[1 - n // ROUNDS, strip_of(n)], out_loc.at[own_sem(n)]
        )

    def out_up(n):
        return og_ref.at[1 - n // ROUNDS, core, strip_of(n), jnp.minimum(kind(n), 1)]

    def out_here(n):
        return pltpu.make_async_copy(W.at[term(n), chip, :, own_rows], out_up(n), out_loc.at[own_sem(n)])

    def out_there(n):
        part = W.at[term(n), chip, :, mate_rows]
        number = 2 * (n // 3) + jnp.minimum(kind(n), 1)
        return remote(part, out_up(n), out_send.at[own_sem(n)], out_recv.at[number], mate)

    def rs_retire(n):
        for way in (0, 1):
            for count in (3, 4):
                @pl.when(hops(n, way) == count)
                def _():
                    sent = W.at[term(n), pl.ds(0, count)]
                    remote(sent, sent, rs_send.at[own_sem(n), way], rs_recv.at[0, way, 0], ring[way]).wait_send()

        @pl.when(kind(n) == 2)
        def _():
            out_down(n).wait()

        @pl.when(kind(n) != 2)
        def _():
            out_here(n).wait()
            out_there(n).wait_send()

    def rs_event(n, h):
        ok = (n >= 0) & (n < ALL)

        @pl.when(ok)
        def _():
            slot = term(n)
            for way in (0, 1):
                @pl.when(h == 0)
                def _():
                    @pl.when(n >= R_SLOTS)
                    def _():
                        pl.semaphore_wait(credit.at[way], 1)

                    rs_copy(n, way, 0).start()

                @pl.when((h > 0) & (h <= hops(n, way)))
                def _():
                    rs_copy(n, way, h - 1).wait_recv()

                    @pl.when(h < hops(n, way))
                    def _():
                        step = hops(n, way) - h
                        own = chip_at(q + step if way == 0 else q - step)
                        total = W[slot, own].astype(F32) + R[came(n, way, h - 1)].astype(F32)
                        W[slot, own] = total.astype(BF16)
                        rs_copy(n, way, h).start()

            @pl.when(h == 4)
            def _():
                total = W[slot, chip].astype(F32) + R[came(n, 0, hops(n, 0) - 1)].astype(F32)
                total = total + R[came(n, 1, hops(n, 1) - 1)].astype(F32)
                W[slot, chip] = total.astype(BF16)

                @pl.when(kind(n) == 2)
                def _():
                    out_down(n).start()

                @pl.when(kind(n) != 2)
                def _():
                    out_here(n).start()
                    out_there(n).start()

                @pl.when(n < ALL - R_SLOTS)
                def _():
                    for way in (0, 1):
                        pl.semaphore_signal(credit.at[way], inc=1, device_id=ring[1 - way], device_id_type=MESH)

    def rs_events(lo, hi):
        def body(e, _):
            h = lax.rem(4 * e, 5)
            rs_event((e - 4 * h) // 5, h)
            return 0

        lax.fori_loop(lo, hi, body, 0)

    block = min(256, tok)
    blocks = 2 * tok // block

    def part(t, size=block):
        return pl.ds(pl.multiple_of(t * size, size), size)

    def normed(h):
        wide = h.astype(F32)
        return (wide * lax.rsqrt(jnp.mean(wide * wide, -1, keepdims=True) + 1e-6)).astype(BF16)

    def norm_block(c, flip):
        def body(t, _):
            s = pl.ds(pl.multiple_of(c * tok + t * block, block), block)
            a = normed(A[s, :])
            A[s, :] = a
            if flip:
                AT[:, s] = a.T
            return 0

        lax.fori_loop(0, tok // block, body, 0)

    def flip_dy(c):
        def body(t, _):
            s = pl.ds(pl.multiple_of(c * tok + t * block, block), block)
            DYT[:, s] = DY[s, :].T
            return 0

        lax.fori_loop(0, tok // block, body, 0)

    def clear():
        def body(t, _):
            ACC[part(t), :] = jnp.zeros((block, d), F32)
            return 0

        lax.fori_loop(0, blocks, body, 0)

    def own_block(t):
        return pl.ds(pl.multiple_of(core * tok + t * block, block), block)

    def nth(t):
        return part(lax.rem(t + 2 * (1 - core), 4), tile)

    def swap(k, t):
        src = ACC.at[pl.ds(pl.multiple_of((1 - core) * tok + t * tile, tile), tile)]
        return remote(src, PT.at[part(t, tile)], sw_send.at[k, t], sw_recv.at[k, t], mate)

    def forward(j, after):
        i, hh = j // 2, lax.rem(j, 2)
        r = 3 * i + 1 + hh

        def body(t, _):
            s = nth(t)
            at = A[s, :]
            gate = nn(at, W[r, :, 0].reshape(d, -1))
            up = nn(at, W[r, :, 1].reshape(d, -1))
            act = (gate * (0.5 * jnp.tanh(0.5 * gate) + 0.5) * up).astype(BF16)
            ACC[s, :] += nn(act, W[3 * i, pl.ds(4 * hh, 4)].reshape(-1, d))

            @pl.when((j == 7) & (t < 2))
            def _():
                swap(0, t).start()

            after(t)
            return 0

        lax.fori_loop(0, 4, body, 0)

    ag_events(0, 1)
    prep_all(3, ROUNDS)
    ag_events(1, 4)
    loaded_up(1)
    prep_all(ROUNDS, ALL)
    load_x.wait()
    norm_block(core, False)
    ag_events(4, 6)
    send_x.wait_recv()
    norm_block(1 - core, False)
    clear()
    ag_events(6, 9)
    load_dy.wait()
    flip_dy(core)
    ag_events(9, 11)
    send_dy.wait_recv()
    flip_dy(1 - core)
    ag_events(11, FIRST[0])

    def first(j, _):
        i, hh = j // 2, lax.rem(j, 2)

        @pl.when(hh == 0)
        def _():
            ag_ready(3 * i)

        ag_ready(3 * i + 1 + hh)
        lo, count = pick(FIRST[:8], j), pick(FIRST[1:], j) - pick(FIRST[:8], j)
        forward(j, lambda t: ag_events(lo + (count * t) // 4, lo + (count * (t + 1)) // 4))
        return 0

    lax.fori_loop(0, 8, first, 0)

    whole = DG.at[pl.ds(0, 4 * ALL // 3 * rows)]
    remote(whole, whole, prep_send, prep_rem.at[0], mate).wait_send()
    fetch = pltpu.make_async_copy(x_ref, DG.at[pl.ds(0, tok)], loc.at[2])
    fetch.start()
    ag_events(55, 57)
    fetch.wait()
    swap(0, 0).wait()
    swap(0, 1).wait()

    def residual(t, _):
        mlp = (ACC[own_block(t), :] + PT[part(t), :]).astype(BF16)
        h = (DG[part(t), :].astype(F32) + mlp.astype(F32)).astype(BF16)
        ACT[part(t), :] = h
        A[own_block(t), :] = h
        return 0

    lax.fori_loop(0, tok // block, residual, 0)
    h1 = ACT.at[pl.ds(0, tok)]
    send_h = remote(h1, A.at[mine], ex_send.at[3], ex_recv.at[3], mate)
    keep_h = pltpu.make_async_copy(h1, h1_ref, loc.at[3])
    send_h.start()
    keep_h.start()
    clear()
    norm_block(core, True)
    ag_events(57, 60)
    send_h.wait()
    norm_block(1 - core, True)
    ag_events(60, 62)
    keep_h.wait()

    def norm_back(h_ref, t):
        by_a = (ACC[own_block(t), :] + PT[part(t), :]).astype(BF16).astype(F32)
        wide = h_ref[part(t), :].astype(F32)
        scale = lax.rsqrt(jnp.mean(wide * wide, -1, keepdims=True) + 1e-6)
        along = jnp.mean(by_a * wide, -1, keepdims=True)
        by_h = (by_a * scale - wide * (scale * scale * scale * along)).astype(BF16)
        return (DY[own_block(t), :].astype(F32) + by_h.astype(F32)).astype(BF16)

    def chunk(c, _):
        l = 1 - c // 8
        j = lax.rem(c, 8)
        i, hh = turn(l, j // 2), lax.rem(j, 2)
        pair = c // 2
        base = ROUNDS * l + 3 * i
        up_slot, down_slot = term(3 * pair + hh), term(3 * pair + 2)

        lo = jnp.where(c == 8, BETWEEN[1], events_by(c))
        count = events_by(c + 1) - lo

        def serve(slot):
            ag_lo, ag_hi = 62 + 8 * c + slot, 63 + 8 * c + slot
            ag_events(jnp.minimum(ag_lo, LAST_AG), jnp.minimum(ag_hi, LAST_AG))
            rs_events(lo + (count * slot) // 8, lo + (count * slot + count) // 8)

        @pl.when(c == 8)
        def _():
            start, end = BETWEEN
            again = pltpu.make_async_copy(x_ref, A.at[mine], loc.at[5])
            again.start()
            send_xp.wait_recv()
            other = pltpu.make_async_copy(xp_ref, A.at[theirs], loc.at[6])
            other.start()
            fetch = pltpu.make_async_copy(h1_ref, DG.at[pl.ds(0, tok)], loc.at[4])
            fetch.start()
            rs_events(start, start + 1)
            fetch.wait()
            swap(1, 0).wait()
            swap(1, 1).wait()

            def body(t, _):
                dh = norm_back(DG, t)
                DY[own_block(t), :] = dh
                ACT[part(t), :] = dh
                return 0

            lax.fori_loop(0, tok // block, body, 0)
            send = remote(ACT.at[pl.ds(0, tok)], DY.at[mine], ex_send.at[4], ex_recv.at[4], mate)
            send.start()
            clear()
            flip_dy(core)
            rs_events(start + 1, start + 2)
            again.wait()
            norm_block(core, True)
            rs_events(start + 2, start + 3)
            other.wait()
            norm_block(1 - core, True)
            rs_events(start + 3, end)
            send.wait()
            flip_dy(1 - core)

            def gone(g, _):
                ag_retire(g)
                return 0

            lax.fori_loop(GATHERED - S_SLOTS, GATHERED, gone, 0)
            across_sent(1)

        @pl.when(l == 1)
        def _():
            @pl.when(hh == 0)
            def _():
                ag_ready(base)

            ag_ready(base + 1 + hh)

        def tokens(t, _):
            s = nth(t)
            at = A[s, :]
            wg, wu = W[base + 1 + hh, :, 0].reshape(d, -1), W[base + 1 + hh, :, 1].reshape(d, -1)
            gate, up = nn(at, wg), nn(at, wu)
            by_act = nt(DY[s, :], W[base, pl.ds(4 * hh, 4)].reshape(-1, d)).astype(BF16).astype(F32)
            sig = 0.5 * jnp.tanh(0.5 * gate) + 0.5
            silu = gate * sig
            ACT[s, :] = (silu * up).astype(BF16)
            dup = (by_act * silu).astype(BF16)
            dgate = (by_act * up * (sig + silu * (1.0 - sig))).astype(BF16)
            DG[s, :] = dgate
            DU[s, :] = dup
            ACC[s, :] += nt(dgate, wg) + nt(dup, wu)

            @pl.when((j == 7) & (t < 2))
            def _():
                swap(2 - l, t).start()

            serve(t)
            return 0

        lax.fori_loop(0, 4, tokens, 0)

        for back, when in ((0, 0), (1, 1), (2, 0)):
            n = 3 * pair + back - T_SLOTS

            @pl.when((hh == when) & (n >= 0))
            def _():
                rs_retire(n)

        def grads_up(p, _):
            s = pl.ds(pl.multiple_of(p * (d // 2), d // 2), d // 2)
            W[up_slot, pl.ds(4 * p, 4), 0] = nn(AT[s, :], DG[...]).astype(BF16).reshape(4, half, -1)
            W[up_slot, pl.ds(4 * p, 4), 1] = nn(AT[s, :], DU[...]).astype(BF16).reshape(4, half, -1)
            serve(4 + p)
            return 0

        lax.fori_loop(0, 2, grads_up, 0)

        for p in range(2):
            s = slice(p * (d // 2), (p + 1) * (d // 2))
            g = nn(DYT[s, :], ACT[...]).T.astype(BF16)
            W[down_slot, pl.ds(4 * hh, 4), :, :, s] = g.reshape(4, 2, half, d // 2)
            serve(6 + p)

        return 0

    lax.fori_loop(0, 16, chunk, 0)

    fetch = pltpu.make_async_copy(x_ref, DG.at[pl.ds(0, tok)], loc.at[7])
    fetch.start()
    rs_events(110, 111)
    fetch.wait()
    swap(2, 0).wait()
    swap(2, 1).wait()

    def last(t, _):
        ACT[part(t), :] = norm_back(DG, t)
        return 0

    lax.fori_loop(0, tok // block, last, 0)
    put = pltpu.make_async_copy(ACT.at[pl.ds(0, tok)], dx_ref, loc.at[8])
    put.start()
    rs_events(111, LAST_RS)

    put.wait()
    for copy in (send_x, send_xp, send_dy):
        copy.wait_send()

    def sent(r, _):
        @pl.when(r >= ALL - T_SLOTS)
        def _():
            rs_retire(r)

        @pl.when(kind(r) != 2)
        def _():
            out_there(r).wait_recv()

        return 0

    across_sent(0)
    lax.fori_loop(0, ALL, sent, 0)


def put_kernel(dx_ref, og_ref, od_ref, dx_out, dwg_out, dwu_out, dwd_out, dx, og, od, dwg, dwu, came, went):
    layers = dwg.shape[0]
    strip = dwg.shape[2] // 64
    loads = [pltpu.make_async_copy(og_ref.at[l], og.at[l], came.at[l]) for l in range(layers)]
    others = [(dx_ref, dx, dx_out), (od_ref, od, dwd_out)]
    for copy in loads:
        copy.start()
    for k, (src, buffer, _) in enumerate(others):
        pltpu.make_async_copy(src, buffer, came.at[2 + k]).start()
    for l in range(layers):
        loads[l].wait()
        for part in range(16):
            c, i, hh = part // 8, part // 2 % 4, part % 2
            for s in range(4):
                column = strip * (8 * (4 * hh + s) + 4 * c + i)
                for g, out in enumerate((dwg, dwu)):
                    out[l, :, column : column + strip] = og[l, c, i, hh, g, :, strip * s : strip * (s + 1)]
        pltpu.make_async_copy(dwg.at[l], dwg_out.at[l], went.at[2 * l]).start()
        pltpu.make_async_copy(dwu.at[l], dwu_out.at[l], went.at[2 * l + 1]).start()
    for k, (src, buffer, dst) in enumerate(others):
        pltpu.make_async_copy(src, buffer, came.at[2 + k]).wait()
        pltpu.make_async_copy(buffer, dst, went.at[4 + k]).start()
    for l in range(layers):
        pltpu.make_async_copy(dwg.at[l], dwg_out.at[l], went.at[2 * l]).wait()
        pltpu.make_async_copy(dwu.at[l], dwu_out.at[l], went.at[2 * l + 1]).wait()
    for k, (_, buffer, dst) in enumerate(others):
        pltpu.make_async_copy(buffer, dst, went.at[4 + k]).wait()


def of_a_device(x, dy, w_gate, w_up, w_down):
    _, tok, d = x.shape
    layers, rows, ff = w_gate.shape
    half = 2 * rows
    strip = ff // 64
    wd = w_down.reshape(layers, 4, 2, half, d)
    hbm = pl.BlockSpec(memory_space=pltpu.HBM)
    tile = tok // 2
    piece = (2, half, d)
    both = 2 * tok
    dma = pltpu.SemaphoreType.DMA
    up = (layers, 2, 4, 2, 2, rows, 4 * strip)
    dx, og, od, _, _ = pl.pallas_call(
        functools.partial(kernel, tile),
        out_shape=tuple(
            jax.ShapeDtypeStruct(shape, BF16)
            for shape in ((tok, d), up, wd.shape, (tok, d), (tok, d))
        ),
        in_specs=[hbm] * 5,
        out_specs=[hbm] * 5,
        scratch_shapes=[
            pltpu.VMEM((ALL + T_SLOTS, 8, *piece), BF16),
            pltpu.VMEM((7 * R_SLOTS, *piece), BF16),
            pltpu.VMEM((both, d), BF16),
            pltpu.VMEM((d, both), BF16),
            pltpu.VMEM((both, d), BF16),
            pltpu.VMEM((d, both), BF16),
            pltpu.VMEM((both, d), F32),
            pltpu.VMEM((tok, d), F32),
            pltpu.VMEM((both, 4 * strip), BF16),
            pltpu.VMEM((both, 4 * strip), BF16),
            pltpu.VMEM((both, 4 * strip), BF16),
            dma((ALL // 3,)),
            dma((layers,)),
            dma(()),
            dma((2 * ALL // 3,)),
            dma((S_SLOTS, 2)),
            dma((S_SLOTS, 2, 4)),
            dma((2,)),
            dma((ALL,)),
            dma((T_SLOTS, 2)),
            dma((R_SLOTS, 2, 4)),
            dma((T_SLOTS,)),
            dma((T_SLOTS,)),
            dma((2 * ALL // 3,)),
            dma((5,)),
            dma((5,)),
            dma((3, 2)),
            dma((3, 2)),
            dma((9,)),
            pltpu.SemaphoreType.REGULAR((2,)),
        ],
        compiler_params=pltpu.CompilerParams(
            collective_id=0, has_side_effects=True, vmem_limit_bytes=67043328
        ),
    )(x[0], dy[0], w_gate, w_up, wd)
    results = (dx.shape, w_gate.shape, w_up.shape, od.shape)
    dx, dwg, dwu, dwd = pl.pallas_call(
        put_kernel,
        out_shape=tuple(jax.ShapeDtypeStruct(shape, BF16) for shape in results),
        in_specs=[hbm] * 3,
        out_specs=[hbm] * 4,
        scratch_shapes=[
            *(pltpu.VMEM(shape, BF16) for shape in (dx.shape, up, od.shape, w_gate.shape, w_up.shape)),
            dma((4,)),
            dma((6,)),
        ],
    )(dx, og, od)
    return dx[None], dwg, dwu, dwd.reshape(w_down.shape)


def solution(mesh):
    by_seq, by_row = P(("rep", "dp"), None, None), P(None, "dp", None)
    out = P("rep", "dp", None)
    return jax.shard_map(
        of_a_device,
        mesh=mesh,
        in_specs=(by_seq, by_seq, by_row, by_row, by_row),
        out_specs=(by_seq, out, out, out),
        check_vma=False,
    )
```

```python
import functools

import jax
import jax.numpy as jnp
from jax import lax
from jax.experimental import pallas as pl
from jax.experimental.pallas import tpu as pltpu
from jax.sharding import PartitionSpec as P

MESH = pl.DeviceIdType.MESH
F32, BF16 = jnp.float32, jnp.bfloat16
ROUNDS = 12
ALL = 2 * ROUNDS
T_SLOTS, R_SLOTS, S_SLOTS = 8, 6, 8
GATHERED = 14
FIRST = (21, 27, 31, 37, 41, 47, 50, 52, 55)
BETWEEN = 45, 51
SECOND = (62, 67, 77, 82, 82)
LAST_AG, LAST_RS = 5 * (GATHERED - 1) + 17, 5 * ALL + 17


def events_by(c):
    return jnp.where(c <= 8, jnp.maximum((13 * c - 14) // 2, jnp.minimum(c, 1)), (15 * c - 19) // 2)


def pick(values, k):
    out = values[-1]
    for number, value in enumerate(values[:-1]):
        out = jnp.where(k == number, value, out)
    return out


def loop(end, body, start=0):
    def step(k, carry):
        body(k)
        return carry

    lax.fori_loop(start, end, step, 0)


def nn(a, b):
    return jnp.dot(a, b, preferred_element_type=F32)


def nt(a, b):
    return lax.dot_general(a, b, (((1,), (1,)), ((), ())), preferred_element_type=F32)


def kernel(tile, x_ref, dy_ref, wg_ref, wu_ref, wd_ref, dx_ref, og_ref, od_ref, xp_ref, h1_ref,
           W, R, A, AT, DY, DYT, ACC, PT, ACT, DG, DU,
           prep_loc, prep_up, prep_send, prep_rem, ag_send, ag_recv, ax_send, ax_recv,
           rs_send, rs_recv, out_loc, out_send, out_recv, ex_send, ex_recv, sw_send, sw_recv, loc, credit):
    tok, d = x_ref.shape
    half = wd_ref.shape[3]
    rows = half // 2
    strip = wg_ref.shape[2] // 64
    assert d == 4 * strip and half == strip // 2
    rep, dp = lax.axis_index("rep"), lax.axis_index("dp")
    core, chip = lax.rem(dp, 2), dp // 2
    q = jnp.where(chip < 4, chip, 11 - chip)

    def chip_at(place):
        place = lax.rem(place + 16, 8)
        return jnp.where(place < 4, place, 11 - place)

    ring = tuple((rep, 2 * chip_at(q + step) + core) for step in (1, -1))
    across, mate = (1 - rep, dp), (rep, 2 * chip + 1 - core)

    def remote(src, dst, send, recv, to):
        return pltpu.make_async_remote_copy(
            src_ref=src, dst_ref=dst, send_sem=send, recv_sem=recv, device_id=to, device_id_type=MESH
        )

    barrier = pltpu.get_barrier_semaphore()
    for other in (*ring, across, mate):
        pl.semaphore_signal(barrier, inc=1, device_id=other, device_id_type=MESH)

    mine, theirs = pl.ds(core * tok, tok), pl.ds((1 - core) * tok, tok)
    own_rows = pl.ds(pl.multiple_of(core * rows, rows), rows)
    mate_rows = pl.ds(pl.multiple_of((1 - core) * rows, rows), rows)

    def kind(r):
        return lax.rem(r, 3)

    def prep_down(r):
        src = wd_ref.at[r // ROUNDS, lax.rem(r, ROUNDS) // 3]
        return pltpu.make_async_copy(src, W.at[r, chip], prep_loc.at[r // 3])

    def staged(l, g, b, columns=slice(None)):
        spot = 16 * g + b
        return 8 * l + spot // 4, lax.rem(spot // 2, 2), pl.ds(pl.multiple_of(rows * lax.rem(spot, 2), rows), rows), columns

    def load_up(l):
        def body(b):
            for g, ref in enumerate((wg_ref, wu_ref)):
                src = ref.at[l, :, pl.ds(pl.multiple_of(d * b, d), d)]
                pltpu.make_async_copy(src, R.at[staged(l, g, b)], prep_up.at[l]).start()

        loop(16, body)

    def loaded_up(l):
        eight = R.at[pl.ds(8 * l, 8)]
        pltpu.make_async_copy(eight, eight, prep_up.at[l]).wait()

    def up_number(r):
        return 2 * (r // 3) + kind(r) - 1

    def mate_part(r, g):
        return pl.ds(pl.multiple_of((2 * up_number(r) + g) * rows, rows), rows)

    def prep_start(r):
        l, i, hh = r // ROUNDS, lax.rem(r, ROUNDS) // 3, kind(r) - 1
        columns = pl.ds(pl.multiple_of(strip * i, strip), strip)
        for g in range(2):
            for s in range(4):
                place = slice(strip * s, strip * (s + 1))
                b = 2 * (4 * hh + s)
                W[r, chip, g, own_rows, place] = R[staged(l, g, b + core, columns)]
                DG[mate_part(r, g), place] = R[staged(l, g, b + 1 - core, columns)]
            dst = W.at[r, chip, g, own_rows]
            remote(DG.at[mate_part(r, g)], dst, prep_send, prep_rem.at[up_number(r)], mate).start()

    def prep_there(r):
        part = W.at[r, chip, :, own_rows]
        return remote(part, part, prep_send, prep_rem.at[up_number(r)], mate)

    def prep_first(r):
        prep_down(3 * r).start()

    load_up(0)
    loop(ALL // 3, prep_first)
    load_up(1)

    def prep_all(lo, hi):
        def body(r):
            @pl.when(kind(r) != 0)
            def _():
                prep_start(r)

        loop(hi, body, lo)

    load_x = pltpu.make_async_copy(x_ref, A.at[mine], loc.at[0])
    load_dy = pltpu.make_async_copy(dy_ref, DY.at[mine], loc.at[1])
    load_x.start()
    load_dy.start()
    pl.semaphore_wait(barrier, 4)

    send_x = remote(x_ref, A.at[mine], ex_send.at[0], ex_recv.at[0], mate)
    send_xp = remote(x_ref, xp_ref, ex_send.at[1], ex_recv.at[1], mate)
    send_dy = remote(dy_ref, DY.at[mine], ex_send.at[2], ex_recv.at[2], mate)
    loaded_up(0)
    prep_all(0, 3)
    send_x.start()
    send_xp.start()
    send_dy.start()

    def wait_prep(r):
        @pl.when(lax.rem(r, 3) == 0)
        def _():
            prep_down(r).wait()

        @pl.when(lax.rem(r, 3) != 0)
        def _():
            prep_there(r).wait_recv()

    def hops(r, way):
        return 4 - lax.rem(r + way + 8, 2)

    def shared(r):
        return (r >= ROUNDS) | (kind(r) != 2)

    def gathers(r):
        first = (kind(r) == 2) | (kind(r) == rep)
        return jnp.where(r < ROUNDS, first, (r - ROUNDS) // 6 == rep)

    def across_number(r):
        return jnp.where(r < ROUNDS, r // 3, 4 + lax.rem(r, 6))

    def gathered(g):
        return jnp.where(
            g < 8, pick((rep, 3 + rep, 2, 6 + rep, 5, 9 + rep, 8, 11), g), ROUNDS + 6 * rep + g - 8
        )

    def ag_copy(g, r, way, h):
        piece = W.at[r, chip_at(q - h if way == 0 else q + h)]
        slot = lax.rem(g, S_SLOTS)
        return remote(piece, piece, ag_send.at[slot, way], ag_recv.at[slot, way, h], ring[way])

    def ag_retire(g):
        for way in (0, 1):
            for count in (3, 4):
                @pl.when(hops(g, way) == count)
                def _():
                    sent = W.at[0, pl.ds(0, count)]
                    remote(sent, sent, ag_send.at[lax.rem(g, S_SLOTS), way], ag_recv.at[0, way, 0], ring[way]).wait_send()

    def ag_event(g, h):
        @pl.when((g >= 0) & (g < GATHERED))
        def _():
            r = gathered(g)

            @pl.when(h == 0)
            def _():
                wait_prep(r)

                @pl.when(g >= S_SLOTS)
                def _():
                    ag_retire(g - S_SLOTS)

            for way in (0, 1):
                @pl.when(h == 0)
                def _():
                    ag_copy(g, r, way, 0).start()

                @pl.when((h > 0) & (h <= hops(g, way)))
                def _():
                    ag_copy(g, r, way, h - 1).wait_recv()

                    @pl.when(h < hops(g, way))
                    def _():
                        ag_copy(g, r, way, h).start()

                    @pl.when(shared(r))
                    def _():
                        piece = W.at[r, chip_at(q - h if way == 0 else q + h)]
                        remote(piece, piece, ax_send.at[r // ROUNDS], ax_recv.at[across_number(r)], across).start()

    def ag_ready(r):
        @pl.when(jnp.logical_not(gathers(r)))
        def _():
            wait_prep(r)
            seven = W.at[r, pl.ds(0, 7)]
            remote(seven, seven, ax_send.at[0], ax_recv.at[across_number(r)], across).wait_recv()

    def across_sent(l):
        some = W.at[pl.ds(0, 7), pl.ds(0, 4)] if l == 0 else W.at[pl.ds(0, 7), pl.ds(0, 6)]
        remote(some, some, ax_send.at[l], ax_recv.at[0], across).wait_send()

    def ag_events(lo, hi):
        def body(e):
            h = lax.rem(4 * e, 5)
            ag_event((e - 4 * h) // 5, h)

        loop(hi, body, lo)

    def turn(l, k):
        return jnp.where(l == 1, lax.rem(k + 2 * rep, 4), k)

    def strip_of(n):
        return turn(1 - n // ROUNDS, lax.rem(n, ROUNDS) // 3)

    def term(n):
        return jnp.where(n < ROUNDS, ALL + lax.rem(n, T_SLOTS), n)

    def own_sem(n):
        return lax.rem(n, T_SLOTS)

    def spot(n, owner, cut):
        return (ALL - 1, owner, n - (ALL - 1)) if cut else (term(n), owner)

    def came(n, way, h, cut):
        place = 7 * lax.rem(n, R_SLOTS) + (h if way == 0 else hops(n, 0) + h)
        return (place, 0) if cut else (place,)

    def rs_copy(n, way, h, cut):
        step = hops(n, way) - h
        return remote(
            W.at[spot(n, chip_at(q + step if way == 0 else q - step), cut)],
            R.at[came(n, way, h, cut)],
            rs_send.at[own_sem(n), way],
            rs_recv.at[lax.rem(n, R_SLOTS), way, h],
            ring[way],
        )

    def out_down(n, cut):
        dst = (0, 3, n - (ALL - 1)) if cut else (1 - n // ROUNDS, strip_of(n))
        return pltpu.make_async_copy(W.at[spot(n, chip, cut)], od_ref.at[dst], out_loc.at[own_sem(n)])

    def out_up(n):
        return og_ref.at[1 - n // ROUNDS, core, strip_of(n), jnp.minimum(kind(n), 1)]

    def out_here(n):
        return pltpu.make_async_copy(W.at[term(n), chip, :, own_rows], out_up(n), out_loc.at[own_sem(n)])

    def out_there(n):
        part = W.at[term(n), chip, :, mate_rows]
        return remote(part, out_up(n), out_send.at[own_sem(n)], out_recv, mate)

    def rs_retire(n, cut=False):
        for way in (0, 1):
            for count in (3, 4):
                @pl.when(hops(n, way) == count)
                def _():
                    sent = W.at[spot(n, pl.ds(0, count), cut)]
                    remote(sent, sent, rs_send.at[own_sem(n), way], rs_recv.at[0, way, 0], ring[way]).wait_send()

        if cut:
            out_down(n, cut).wait()
            return

        @pl.when(kind(n) == 2)
        def _():
            out_down(n, cut).wait()

        @pl.when(kind(n) != 2)
        def _():
            out_here(n).wait()
            out_there(n).wait_send()

    def rs_event(n, h, cut):
        for way in (0, 1):
            @pl.when(h == 0)
            def _():
                @pl.when(n >= R_SLOTS)
                def _():
                    pl.semaphore_wait(credit.at[way], 1)

                rs_copy(n, way, 0, cut).start()

            @pl.when((h > 0) & (h <= hops(n, way)))
            def _():
                rs_copy(n, way, h - 1, cut).wait_recv()

                @pl.when(h < hops(n, way))
                def _():
                    step = hops(n, way) - h
                    own = spot(n, chip_at(q + step if way == 0 else q - step), cut)
                    total = W[own].astype(F32) + R[came(n, way, h - 1, cut)].astype(F32)
                    W[own] = total.astype(BF16)
                    rs_copy(n, way, h, cut).start()

        @pl.when(h == 4)
        def _():
            own = spot(n, chip, cut)
            total = W[own].astype(F32) + R[came(n, 0, hops(n, 0) - 1, cut)].astype(F32)
            total = total + R[came(n, 1, hops(n, 1) - 1, cut)].astype(F32)
            W[own] = total.astype(BF16)
            if cut:
                out_down(n, cut).start()
                return

            @pl.when(kind(n) == 2)
            def _():
                out_down(n, cut).start()

            @pl.when(kind(n) != 2)
            def _():
                out_here(n).start()
                out_there(n).start()

            @pl.when(n <= ALL - R_SLOTS)
            def _():
                for way in (0, 1):
                    pl.semaphore_signal(credit.at[way], inc=1, device_id=ring[1 - way], device_id_type=MESH)

    def rs_events(lo, hi, end=False):
        def body(e):
            h = lax.rem(4 * e, 5)
            n = (e - 4 * h) // 5

            @pl.when((n >= 0) & (n < ALL - 1))
            def _():
                rs_event(n, h, False)

            if end:
                @pl.when((n >= ALL - 1) & (n <= ALL))
                def _():
                    rs_event(n, h, True)

        loop(hi, body, lo)

    block = min(256, tok)
    blocks = 2 * tok // block

    def part(t, size=block):
        return pl.ds(pl.multiple_of(t * size, size), size)

    def normed(h):
        wide = h.astype(F32)
        return (wide * lax.rsqrt(jnp.mean(wide * wide, -1, keepdims=True) + 1e-6)).astype(BF16)

    def block_of(c, t):
        return pl.ds(pl.multiple_of(c * tok + t * block, block), block)

    def norm_block(c, flip):
        def body(t):
            s = block_of(c, t)
            a = normed(A[s, :])
            A[s, :] = a
            if flip:
                AT[:, s] = a.T

        loop(tok // block, body)

    def flip_dy(c):
        def body(t):
            s = block_of(c, t)
            DYT[:, s] = DY[s, :].T

        loop(tok // block, body)

    def clear():
        def body(t):
            ACC[part(t), :] = jnp.zeros((block, d), F32)

        loop(blocks, body)

    def own_block(t):
        return block_of(core, t)

    def nth(t):
        return part(lax.rem(t + 2 * (1 - core), 4), tile)

    def swap(k, t):
        src = ACC.at[pl.ds(pl.multiple_of((1 - core) * tok + t * tile, tile), tile)]
        return remote(src, PT.at[part(t, tile)], sw_send.at[k, t], sw_recv.at[k, t], mate)

    def forward(j, after):
        i, hh = j // 2, lax.rem(j, 2)
        r = 3 * i + 1 + hh

        def body(t):
            s = nth(t)
            at = A[s, :]
            gate = nn(at, W[r, :, 0].reshape(d, -1))
            up = nn(at, W[r, :, 1].reshape(d, -1))
            act = (gate * (0.5 * jnp.tanh(0.5 * gate) + 0.5) * up).astype(BF16)
            ACC[s, :] += nn(act, W[3 * i, pl.ds(4 * hh, 4)].reshape(-1, d))

            @pl.when((j == 7) & (t < 2))
            def _():
                swap(0, t).start()

            after(t)

        loop(4, body)

    ag_events(0, 1)
    prep_all(3, ROUNDS)
    ag_events(1, 4)
    loaded_up(1)
    prep_all(ROUNDS, ALL)
    load_x.wait()
    norm_block(core, False)
    ag_events(4, 6)
    send_x.wait_recv()
    norm_block(1 - core, False)
    clear()
    ag_events(6, 9)
    load_dy.wait()
    flip_dy(core)
    ag_events(9, 11)
    send_dy.wait_recv()
    flip_dy(1 - core)
    ag_events(11, FIRST[0])

    def first(j):
        i, hh = j // 2, lax.rem(j, 2)

        @pl.when(hh == 0)
        def _():
            ag_ready(3 * i)

        ag_ready(3 * i + 1 + hh)
        lo, count = pick(FIRST[:8], j), pick(FIRST[1:], j) - pick(FIRST[:8], j)
        forward(j, lambda t: ag_events(lo + (count * t) // 4, lo + (count * (t + 1)) // 4))

    loop(8, first)

    whole = DG.at[pl.ds(0, 4 * ALL // 3 * rows)]
    remote(whole, whole, prep_send, prep_rem.at[0], mate).wait_send()
    fetch = pltpu.make_async_copy(x_ref, DG.at[pl.ds(0, tok)], loc.at[2])
    fetch.start()
    ag_events(55, 57)
    fetch.wait()
    swap(0, 0).wait()
    swap(0, 1).wait()

    def residual(t):
        mlp = (ACC[own_block(t), :] + PT[part(t), :]).astype(BF16)
        h = (DG[part(t), :].astype(F32) + mlp.astype(F32)).astype(BF16)
        ACT[part(t), :] = h
        A[own_block(t), :] = h

    loop(tok // block, residual)
    h1 = ACT.at[pl.ds(0, tok)]
    send_h = remote(h1, A.at[mine], ex_send.at[3], ex_recv.at[3], mate)
    keep_h = pltpu.make_async_copy(h1, h1_ref, loc.at[3])
    send_h.start()
    keep_h.start()
    clear()
    norm_block(core, True)
    ag_events(57, 60)
    send_h.wait()
    norm_block(1 - core, True)
    ag_events(60, 62)
    keep_h.wait()

    def norm_back(h_ref, t):
        by_a = (ACC[own_block(t), :] + PT[part(t), :]).astype(BF16).astype(F32)
        wide = h_ref[part(t), :].astype(F32)
        scale = lax.rsqrt(jnp.mean(wide * wide, -1, keepdims=True) + 1e-6)
        along = jnp.mean(by_a * wide, -1, keepdims=True)
        by_h = (by_a * scale - wide * (scale * scale * scale * along)).astype(BF16)
        return (DY[own_block(t), :].astype(F32) + by_h.astype(F32)).astype(BF16)

    def chunk(c):
        l = 1 - c // 8
        j = lax.rem(c, 8)
        i, hh = turn(l, j // 2), lax.rem(j, 2)
        pair = c // 2
        base = ROUNDS * l + 3 * i
        up_slot, down_slot = term(3 * pair + hh), term(3 * pair + 2)

        lo = jnp.where(c == 8, BETWEEN[1], events_by(c))
        count = events_by(c + 1) - lo

        ag_lo, ag_count = pick(SECOND[:-1], c), pick((*SECOND[1:], LAST_AG), c) - pick(SECOND[:-1], c)

        def serve(slot):
            ag_events(ag_lo + (ag_count * slot) // 8, ag_lo + (ag_count * slot + ag_count) // 8)
            rs_events(lo + (count * slot) // 8, lo + (count * slot + count) // 8)

        @pl.when(c == 8)
        def _():
            start, end = BETWEEN
            again = pltpu.make_async_copy(x_ref, A.at[mine], loc.at[5])
            again.start()
            send_xp.wait_recv()
            other = pltpu.make_async_copy(xp_ref, A.at[theirs], loc.at[6])
            other.start()
            fetch = pltpu.make_async_copy(h1_ref, DG.at[pl.ds(0, tok)], loc.at[4])
            fetch.start()
            rs_events(start, start + 1)
            fetch.wait()
            swap(1, 0).wait()
            swap(1, 1).wait()

            def body(t):
                dh = norm_back(DG, t)
                DY[own_block(t), :] = dh
                ACT[part(t), :] = dh

            loop(tok // block, body)
            send = remote(ACT.at[pl.ds(0, tok)], DY.at[mine], ex_send.at[4], ex_recv.at[4], mate)
            send.start()
            clear()
            flip_dy(core)
            rs_events(start + 1, start + 2)
            again.wait()
            norm_block(core, True)
            rs_events(start + 2, start + 3)
            other.wait()
            norm_block(1 - core, True)
            rs_events(start + 3, end)
            send.wait()
            flip_dy(1 - core)

            def gone(g):
                ag_retire(g)

            loop(GATHERED, gone, GATHERED - S_SLOTS)
            across_sent(1)

        @pl.when(l == 1)
        def _():
            @pl.when(hh == 0)
            def _():
                ag_ready(base)

            ag_ready(base + 1 + hh)

        def tokens(t):
            s = nth(t)
            at = A[s, :]
            wg, wu = W[base + 1 + hh, :, 0].reshape(d, -1), W[base + 1 + hh, :, 1].reshape(d, -1)
            gate, up = nn(at, wg), nn(at, wu)
            by_act = nt(DY[s, :], W[base, pl.ds(4 * hh, 4)].reshape(-1, d)).astype(BF16).astype(F32)
            sig = 0.5 * jnp.tanh(0.5 * gate) + 0.5
            silu = gate * sig
            ACT[s, :] = (silu * up).astype(BF16)
            dup = (by_act * silu).astype(BF16)
            dgate = (by_act * up * (sig + silu * (1.0 - sig))).astype(BF16)
            DG[s, :] = dgate
            DU[s, :] = dup
            ACC[s, :] += nt(dgate, wg) + nt(dup, wu)

            @pl.when((j == 7) & (t < 2))
            def _():
                swap(2 - l, t).start()

            serve(t)

        loop(4, tokens)

        for back, when in ((0, 0), (1, 1), (2, 0)):
            n = 3 * pair + back - T_SLOTS

            @pl.when((hh == when) & (n >= 0))
            def _():
                rs_retire(n)

        def grads_up(p):
            s = pl.ds(pl.multiple_of(p * (d // 2), d // 2), d // 2)
            W[up_slot, pl.ds(4 * p, 4), 0] = nn(AT[s, :], DG[...]).astype(BF16).reshape(4, half, -1)
            W[up_slot, pl.ds(4 * p, 4), 1] = nn(AT[s, :], DU[...]).astype(BF16).reshape(4, half, -1)
            serve(4 + p)

        loop(2, grads_up)

        for p in range(2):
            s = slice(p * (d // 2), (p + 1) * (d // 2))
            g = nn(DYT[s, :], ACT[...]).T.astype(BF16)
            W[down_slot, pl.ds(4 * hh, 4), :, :, s] = g.reshape(4, 2, half, d // 2)
            serve(6 + p)

    loop(16, chunk)

    fetch = pltpu.make_async_copy(x_ref, DG.at[pl.ds(0, tok)], loc.at[7])
    fetch.start()
    rs_events(110, 111)
    fetch.wait()
    swap(2, 0).wait()
    swap(2, 1).wait()

    def last(t):
        ACT[part(t), :] = norm_back(DG, t)

    loop(tok // block, last)
    put = pltpu.make_async_copy(ACT.at[pl.ds(0, tok)], dx_ref, loc.at[8])
    put.start()
    rs_retire(ALL - T_SLOTS)
    rs_events(111, LAST_RS, True)

    put.wait()
    for copy in (send_x, send_xp, send_dy):
        copy.wait_send()

    def sent(n):
        rs_retire(n)

    for n in (ALL - 1, ALL):
        rs_retire(jnp.int32(n), True)
    across_sent(0)
    loop(ALL - 1, sent, ALL - T_SLOTS + 1)
    ups = W.at[0]
    remote(ups, ups, out_send.at[0], out_recv, mate).wait_recv()


def put_kernel(dx_ref, og_ref, od_ref, dx_out, dwg_out, dwu_out, dwd_out, dx, og, od, dwg, dwu, came, went):
    layers, _, ff = dwg.shape
    strip = ff // 64

    def copies(pairs, sems):
        return [pltpu.make_async_copy(src, dst, sems.at[k]) for k, (src, dst) in enumerate(pairs)]

    each = range(layers)
    loads = copies([(dx_ref, dx), (od_ref, od)] + [(og_ref.at[l], og.at[l]) for l in each], came)
    stores = [(dx, dx_out), (od, dwd_out)]
    stores = copies(stores + [(a.at[l], b.at[l]) for l in each for a, b in ((dwg, dwg_out), (dwu, dwu_out))], went)
    first = loads[:layers], stores[:layers]
    for copy in loads:
        copy.start()
    for load, store in zip(*first, strict=True):
        load.wait()
        store.start()
    for l in each:
        loads[layers + l].wait()
        for part in range(16):
            c, i, hh = part // 8, part // 2 % 4, part % 2
            for s in range(4):
                column = strip * (8 * (4 * hh + s) + 4 * c + i)
                for g, out in enumerate((dwg, dwu)):
                    out[l, :, column : column + strip] = og[l, c, i, hh, g, :, strip * s : strip * (s + 1)]
        for store in stores[2 * (l + 1) : 2 * (l + 2)]:
            store.start()
    for store in stores:
        store.wait()


def of_a_device(x, dy, w_gate, w_up, w_down):
    _, tok, d = x.shape
    layers, rows, ff = w_gate.shape
    half = 2 * rows
    strip = ff // 64
    wd = w_down.reshape(layers, 4, 2, half, d)
    hbm = pl.BlockSpec(memory_space=pltpu.HBM)
    tile = tok // 2
    piece = (2, half, d)
    both = 2 * tok
    dma = pltpu.SemaphoreType.DMA
    up = (layers, 2, 4, 2, 2, rows, 4 * strip)
    dx, og, od, _, _ = pl.pallas_call(
        functools.partial(kernel, tile),
        out_shape=tuple(
            jax.ShapeDtypeStruct(shape, BF16)
            for shape in ((tok, d), up, wd.shape, (tok, d), (tok, d))
        ),
        in_specs=[hbm] * 5,
        out_specs=[hbm] * 5,
        scratch_shapes=[
            pltpu.VMEM((ALL + T_SLOTS, 8, *piece), BF16),
            pltpu.VMEM((7 * R_SLOTS, *piece), BF16),
            pltpu.VMEM((both, d), BF16),
            pltpu.VMEM((d, both), BF16),
            pltpu.VMEM((both, d), BF16),
            pltpu.VMEM((d, both), BF16),
            pltpu.VMEM((both, d), F32),
            pltpu.VMEM((tok, d), F32),
            pltpu.VMEM((both, 4 * strip), BF16),
            pltpu.VMEM((both, 4 * strip), BF16),
            pltpu.VMEM((both, 4 * strip), BF16),
            dma((ALL // 3,)),
            dma((layers,)),
            dma(()),
            dma((2 * ALL // 3,)),
            dma((S_SLOTS, 2)),
            dma((S_SLOTS, 2, 4)),
            dma((2,)),
            dma((10,)),
            dma((T_SLOTS, 2)),
            dma((R_SLOTS, 2, 4)),
            dma((T_SLOTS,)),
            dma((T_SLOTS,)),
            dma(()),
            dma((5,)),
            dma((5,)),
            dma((3, 2)),
            dma((3, 2)),
            dma((9,)),
            pltpu.SemaphoreType.REGULAR((2,)),
        ],
        compiler_params=pltpu.CompilerParams(
            collective_id=0, has_side_effects=True, vmem_limit_bytes=67043328
        ),
    )(x[0], dy[0], w_gate, w_up, wd)
    results = (dx.shape, w_gate.shape, w_up.shape, od.shape)
    dx, dwg, dwu, dwd = pl.pallas_call(
        put_kernel,
        out_shape=tuple(jax.ShapeDtypeStruct(shape, BF16) for shape in results),
        in_specs=[hbm] * 3,
        out_specs=[hbm] * 4,
        scratch_shapes=[
            *(pltpu.VMEM(shape, BF16) for shape in (dx.shape, up, od.shape, w_gate.shape, w_up.shape)),
            dma((4,)),
            dma((6,)),
        ],
    )(dx, og, od)
    return dx[None], dwg, dwu, dwd.reshape(w_down.shape)


def solution(mesh):
    by_seq, by_row = P(("rep", "dp"), None, None), P(None, "dp", None)
    out = P("rep", "dp", None)
    return jax.shard_map(
        of_a_device,
        mesh=mesh,
        in_specs=(by_seq, by_seq, by_row, by_row, by_row),
        out_specs=(by_seq, out, out, out),
        check_vma=False,
    )
```

```python
import functools

import jax
import jax.numpy as jnp
from jax import lax
from jax.experimental import pallas as pl
from jax.experimental.pallas import tpu as pltpu
from jax.sharding import PartitionSpec as P

MESH = pl.DeviceIdType.MESH
F32, BF16 = jnp.float32, jnp.bfloat16
ROUNDS = 12
ALL = 2 * ROUNDS
T_SLOTS, R_SLOTS, S_SLOTS = 8, 6, 6
GATHERED = 14
FIRST = (21, 27, 31, 37, 41, 47, 50, 52, 55)
BETWEEN = 45, 51
SECOND = (62, 67, 77, 82, 82)
LAST_AG, LAST_RS = 5 * (GATHERED - 1) + 17, 5 * ALL + 17


def events_by(c):
    return jnp.where(c <= 8, jnp.maximum((13 * c - 14) // 2, jnp.minimum(c, 1)), (15 * c - 19) // 2)


def pick(values, k):
    out = values[-1]
    for number, value in enumerate(values[:-1]):
        out = jnp.where(k == number, value, out)
    return out


def loop(end, body, start=0):
    def step(k, carry):
        body(k)
        return carry

    lax.fori_loop(start, end, step, 0)


def nn(a, b):
    return jnp.dot(a, b, preferred_element_type=F32)


def nt(a, b):
    return lax.dot_general(a, b, (((1,), (1,)), ((), ())), preferred_element_type=F32)


def kernel(tile, x_ref, dy_ref, wg_ref, wu_ref, wd_ref, dx_ref, og_ref, od_ref, xp_ref, h1_ref,
           W, R, A, AT, DY, DYT, ACC, PT, ACT, DG, DU,
           prep_loc, prep_up, prep_send, prep_rem, ag_send, ag_recv, ax_send, ax_recv,
           rs_send, rs_recv, out_loc, out_send, out_recv, ex_send, ex_recv, sw_send, sw_recv, loc, credit):
    tok, d = x_ref.shape
    half = wd_ref.shape[3]
    rows = half // 2
    strip = wg_ref.shape[2] // 64
    assert d == 4 * strip and half == strip // 2
    rep, dp = lax.axis_index("rep"), lax.axis_index("dp")
    core, chip = lax.rem(dp, 2), dp // 2
    q = jnp.where(chip < 4, chip, 11 - chip)

    def chip_at(place):
        place = lax.rem(place + 16, 8)
        return jnp.where(place < 4, place, 11 - place)

    ring = tuple((rep, 2 * chip_at(q + step) + core) for step in (1, -1))
    across, mate = (1 - rep, dp), (rep, 2 * chip + 1 - core)

    def remote(src, dst, send, recv, to):
        return pltpu.make_async_remote_copy(
            src_ref=src, dst_ref=dst, send_sem=send, recv_sem=recv, device_id=to, device_id_type=MESH
        )

    barrier = pltpu.get_barrier_semaphore()
    for other in (*ring, across, mate):
        pl.semaphore_signal(barrier, inc=1, device_id=other, device_id_type=MESH)

    mine, theirs = pl.ds(core * tok, tok), pl.ds((1 - core) * tok, tok)
    own_rows = pl.ds(pl.multiple_of(core * rows, rows), rows)
    mate_rows = pl.ds(pl.multiple_of((1 - core) * rows, rows), rows)

    def kind(r):
        return lax.rem(r, 3)

    def prep_down(r):
        src = wd_ref.at[r // ROUNDS, lax.rem(r, ROUNDS) // 3]
        return pltpu.make_async_copy(src, W.at[r, chip], prep_loc.at[r // 3])

    def staged(l, g, b, columns=slice(None)):
        spot = 16 * g + b
        return 8 * l + spot // 4, lax.rem(spot // 2, 2), pl.ds(pl.multiple_of(rows * lax.rem(spot, 2), rows), rows), columns

    def load_up(l):
        def body(b):
            for g, ref in enumerate((wg_ref, wu_ref)):
                src = ref.at[l, :, pl.ds(pl.multiple_of(d * b, d), d)]
                pltpu.make_async_copy(src, R.at[staged(l, g, b)], prep_up.at[l]).start()

        loop(16, body)

    def loaded_up(l):
        eight = R.at[pl.ds(8 * l, 8)]
        pltpu.make_async_copy(eight, eight, prep_up.at[l]).wait()

    def up_number(r):
        return 2 * (r // 3) + kind(r) - 1

    def mate_part(r, g):
        return pl.ds(pl.multiple_of((2 * up_number(r) + g) * rows, rows), rows)

    def prep_start(r):
        l, i, hh = r // ROUNDS, lax.rem(r, ROUNDS) // 3, kind(r) - 1
        columns = pl.ds(pl.multiple_of(strip * i, strip), strip)
        for g in range(2):
            for s in range(4):
                place = slice(strip * s, strip * (s + 1))
                b = 2 * (4 * hh + s)
                W[r, chip, g, own_rows, place] = R[staged(l, g, b + core, columns)]
                DG[mate_part(r, g), place] = R[staged(l, g, b + 1 - core, columns)]
            dst = W.at[r, chip, g, own_rows]
            remote(DG.at[mate_part(r, g)], dst, prep_send, prep_rem.at[up_number(r)], mate).start()

    def prep_there(r):
        part = W.at[r, chip, :, own_rows]
        return remote(part, part, prep_send, prep_rem.at[up_number(r)], mate)

    def prep_first(r):
        prep_down(3 * r).start()

    load_up(0)
    loop(ALL // 3, prep_first)
    load_up(1)

    def prep_all(lo, hi):
        def body(r):
            @pl.when(kind(r) != 0)
            def _():
                prep_start(r)

        loop(hi, body, lo)

    load_x = pltpu.make_async_copy(x_ref, A.at[mine], loc.at[0])
    load_dy = pltpu.make_async_copy(dy_ref, DY.at[mine], loc.at[1])
    load_x.start()
    load_dy.start()
    pl.semaphore_wait(barrier, 4)

    send_x = remote(x_ref, A.at[mine], ex_send.at[0], ex_recv.at[0], mate)
    send_xp = remote(x_ref, xp_ref, ex_send.at[1], ex_recv.at[1], mate)
    send_dy = remote(dy_ref, DY.at[mine], ex_send.at[2], ex_recv.at[2], mate)
    loaded_up(0)
    prep_all(0, 3)
    send_x.start()
    send_xp.start()
    send_dy.start()

    def wait_prep(r):
        @pl.when(lax.rem(r, 3) == 0)
        def _():
            prep_down(r).wait()

        @pl.when(lax.rem(r, 3) != 0)
        def _():
            prep_there(r).wait_recv()

    def hops(r, way):
        return 4 - lax.rem(r + way + 8, 2)

    def shared(r):
        return (r >= ROUNDS) | (kind(r) != 2)

    def gathers(r):
        first = (kind(r) == 2) | (kind(r) == rep)
        return jnp.where(r < ROUNDS, first, (r - ROUNDS) // 6 == rep)

    def across_number(r):
        return jnp.where(r < ROUNDS, r // 3, 4 + lax.rem(r, 6))

    def gathered(g):
        return jnp.where(
            g < 8, pick((rep, 3 + rep, 2, 6 + rep, 5, 9 + rep, 8, 11), g), ROUNDS + 6 * rep + g - 8
        )

    def ag_copy(g, r, way, h):
        piece = W.at[r, chip_at(q - h if way == 0 else q + h)]
        slot = lax.rem(g, S_SLOTS)
        return remote(piece, piece, ag_send.at[slot, way], ag_recv.at[slot, way, h], ring[way])

    def ag_retire(g):
        for way in (0, 1):
            for count in (3, 4):
                @pl.when(hops(g, way) == count)
                def _():
                    sent = W.at[0, pl.ds(0, count)]
                    remote(sent, sent, ag_send.at[lax.rem(g, S_SLOTS), way], ag_recv.at[0, way, 0], ring[way]).wait_send()

    def ag_event(g, h):
        @pl.when((g >= 0) & (g < GATHERED))
        def _():
            r = gathered(g)

            @pl.when(h == 0)
            def _():
                wait_prep(r)

                @pl.when(g >= S_SLOTS)
                def _():
                    ag_retire(g - S_SLOTS)

            for way in (0, 1):
                @pl.when(h == 0)
                def _():
                    ag_copy(g, r, way, 0).start()

                @pl.when((h > 0) & (h <= hops(g, way)))
                def _():
                    ag_copy(g, r, way, h - 1).wait_recv()

                    @pl.when(h < hops(g, way))
                    def _():
                        ag_copy(g, r, way, h).start()

                    @pl.when(shared(r))
                    def _():
                        piece = W.at[r, chip_at(q - h if way == 0 else q + h)]
                        remote(piece, piece, ax_send.at[r // ROUNDS], ax_recv.at[across_number(r)], across).start()

    def ag_ready(r):
        @pl.when(jnp.logical_not(gathers(r)))
        def _():
            wait_prep(r)
            seven = W.at[r, pl.ds(0, 7)]
            remote(seven, seven, ax_send.at[0], ax_recv.at[across_number(r)], across).wait_recv()

    def across_sent(l):
        some = W.at[pl.ds(0, 7), pl.ds(0, 4)] if l == 0 else W.at[pl.ds(0, 7), pl.ds(0, 6)]
        remote(some, some, ax_send.at[l], ax_recv.at[0], across).wait_send()

    def ag_events(lo, hi):
        def body(e):
            h = lax.rem(4 * e, 5)
            ag_event((e - 4 * h) // 5, h)

        loop(hi, body, lo)

    def turn(l, k):
        return jnp.where(l == 1, lax.rem(k + 2 * rep, 4), k)

    def strip_of(n):
        return turn(1 - n // ROUNDS, lax.rem(n, ROUNDS) // 3)

    def term(n):
        return jnp.where(n < ROUNDS, ALL + lax.rem(n, T_SLOTS), n)

    def own_sem(n):
        return lax.rem(n, T_SLOTS)

    def spot(n, owner, cut):
        return (ALL - 1, owner, n - (ALL - 1)) if cut else (term(n), owner)

    def came(n, way, h, cut):
        place = 7 * lax.rem(n, R_SLOTS) + (h if way == 0 else hops(n, 0) + h)
        return (place, 0) if cut else (place,)

    def rs_copy(n, way, h, cut):
        step = hops(n, way) - h
        return remote(
            W.at[spot(n, chip_at(q + step if way == 0 else q - step), cut)],
            R.at[came(n, way, h, cut)],
            rs_send.at[own_sem(n), way],
            rs_recv.at[lax.rem(n, R_SLOTS), way, h],
            ring[way],
        )

    def out_down(n, cut):
        dst = (0, 3, n - (ALL - 1)) if cut else (1 - n // ROUNDS, strip_of(n))
        return pltpu.make_async_copy(W.at[spot(n, chip, cut)], od_ref.at[dst], out_loc.at[own_sem(n)])

    def out_up(n):
        return og_ref.at[1 - n // ROUNDS, core, strip_of(n), jnp.minimum(kind(n), 1)]

    def out_here(n):
        return pltpu.make_async_copy(W.at[term(n), chip, :, own_rows], out_up(n), out_loc.at[own_sem(n)])

    def out_there(n):
        part = W.at[term(n), chip, :, mate_rows]
        return remote(part, out_up(n), out_send.at[own_sem(n)], out_recv, mate)

    def rs_retire(n, cut=False):
        for way in (0, 1):
            for count in (3, 4):
                @pl.when(hops(n, way) == count)
                def _():
                    sent = W.at[spot(n, pl.ds(0, count), cut)]
                    remote(sent, sent, rs_send.at[own_sem(n), way], rs_recv.at[0, way, 0], ring[way]).wait_send()

        if cut:
            out_down(n, cut).wait()
            return

        @pl.when(kind(n) == 2)
        def _():
            out_down(n, cut).wait()

        @pl.when(kind(n) != 2)
        def _():
            out_here(n).wait()
            out_there(n).wait_send()

    def rs_event(n, h, cut):
        for way in (0, 1):
            @pl.when(h == 0)
            def _():
                @pl.when(n >= R_SLOTS)
                def _():
                    pl.semaphore_wait(credit.at[way], 1)

                rs_copy(n, way, 0, cut).start()

            @pl.when((h > 0) & (h <= hops(n, way)))
            def _():
                rs_copy(n, way, h - 1, cut).wait_recv()

                @pl.when(h < hops(n, way))
                def _():
                    step = hops(n, way) - h
                    own = spot(n, chip_at(q + step if way == 0 else q - step), cut)
                    total = W[own].astype(F32) + R[came(n, way, h - 1, cut)].astype(F32)
                    W[own] = total.astype(BF16)
                    rs_copy(n, way, h, cut).start()

        @pl.when(h == 4)
        def _():
            own = spot(n, chip, cut)
            total = W[own].astype(F32) + R[came(n, 0, hops(n, 0) - 1, cut)].astype(F32)
            total = total + R[came(n, 1, hops(n, 1) - 1, cut)].astype(F32)
            W[own] = total.astype(BF16)
            if cut:
                out_down(n, cut).start()
                return

            @pl.when(kind(n) == 2)
            def _():
                out_down(n, cut).start()

            @pl.when(kind(n) != 2)
            def _():
                out_here(n).start()
                out_there(n).start()

            @pl.when(n <= ALL - R_SLOTS)
            def _():
                for way in (0, 1):
                    pl.semaphore_signal(credit.at[way], inc=1, device_id=ring[1 - way], device_id_type=MESH)

    def rs_events(lo, hi, end=False):
        def body(e):
            h = lax.rem(4 * e, 5)
            n = (e - 4 * h) // 5

            @pl.when((n >= 0) & (n < ALL - 1))
            def _():
                rs_event(n, h, False)

            if end:
                @pl.when((n >= ALL - 1) & (n <= ALL))
                def _():
                    rs_event(n, h, True)

        loop(hi, body, lo)

    block = min(256, tok)
    blocks = 2 * tok // block

    def part(t, size=block):
        return pl.ds(pl.multiple_of(t * size, size), size)

    def normed(h):
        wide = h.astype(F32)
        return (wide * lax.rsqrt(jnp.mean(wide * wide, -1, keepdims=True) + 1e-6)).astype(BF16)

    def block_of(c, t):
        return pl.ds(pl.multiple_of(c * tok + t * block, block), block)

    def norm_block(c, flip):
        def body(t):
            s = block_of(c, t)
            a = normed(A[s, :])
            A[s, :] = a
            if flip:
                AT[:, s] = a.T

        loop(tok // block, body)

    def flip_dy(c):
        def body(t):
            s = block_of(c, t)
            DYT[:, s] = DY[s, :].T

        loop(tok // block, body)

    def clear():
        def body(t):
            ACC[part(t), :] = jnp.zeros((block, d), F32)

        loop(blocks, body)

    def own_block(t):
        return block_of(core, t)

    def nth(t):
        return part(lax.rem(t + 2 * (1 - core), 4), tile)

    def swap(t):
        src = ACC.at[pl.ds(pl.multiple_of((1 - core) * tok + t * tile, tile), tile)]
        return remote(src, PT.at[part(t, tile)], sw_send.at[t], sw_recv.at[t], mate)

    def forward(j, after):
        i, hh = j // 2, lax.rem(j, 2)
        r = 3 * i + 1 + hh

        def body(t):
            s = nth(t)
            at = A[s, :]
            gate = nn(at, W[r, :, 0].reshape(d, -1))
            up = nn(at, W[r, :, 1].reshape(d, -1))
            act = (gate * (0.5 * jnp.tanh(0.5 * gate) + 0.5) * up).astype(BF16)
            ACC[s, :] += nn(act, W[3 * i, pl.ds(4 * hh, 4)].reshape(-1, d))

            @pl.when((j == 7) & (t < 2))
            def _():
                swap(t).start()

            after(t)

        loop(4, body)

    ag_events(0, 1)
    prep_all(3, ROUNDS)
    ag_events(1, 4)
    loaded_up(1)
    prep_all(ROUNDS, ALL)
    load_x.wait()
    norm_block(core, False)
    ag_events(4, 6)
    send_x.wait_recv()
    norm_block(1 - core, False)
    clear()
    ag_events(6, 9)
    load_dy.wait()
    flip_dy(core)
    ag_events(9, 11)
    send_dy.wait_recv()
    flip_dy(1 - core)
    ag_events(11, FIRST[0])

    def first(j):
        i, hh = j // 2, lax.rem(j, 2)

        @pl.when(hh == 0)
        def _():
            ag_ready(3 * i)

        ag_ready(3 * i + 1 + hh)
        lo, count = pick(FIRST[:8], j), pick(FIRST[1:], j) - pick(FIRST[:8], j)
        forward(j, lambda t: ag_events(lo + (count * t) // 4, lo + (count * (t + 1)) // 4))

    loop(8, first)

    whole = DG.at[pl.ds(0, 4 * ALL // 3 * rows)]
    remote(whole, whole, prep_send, prep_rem.at[0], mate).wait_send()
    fetch = pltpu.make_async_copy(x_ref, DG.at[pl.ds(0, tok)], loc.at[0])
    fetch.start()
    ag_events(55, 57)
    fetch.wait()
    swap(0).wait()
    swap(1).wait()

    def residual(t):
        mlp = (ACC[own_block(t), :] + PT[part(t), :]).astype(BF16)
        h = (DG[part(t), :].astype(F32) + mlp.astype(F32)).astype(BF16)
        ACT[part(t), :] = h
        A[own_block(t), :] = h

    loop(tok // block, residual)
    h1 = ACT.at[pl.ds(0, tok)]
    send_h = remote(h1, A.at[mine], ex_send.at[3], ex_recv.at[3], mate)
    keep_h = pltpu.make_async_copy(h1, h1_ref, loc.at[1])
    send_h.start()
    keep_h.start()
    clear()
    norm_block(core, True)
    ag_events(57, 60)
    send_h.wait()
    norm_block(1 - core, True)
    ag_events(60, 62)
    keep_h.wait()

    def norm_back(h_ref, t):
        by_a = (ACC[own_block(t), :] + PT[part(t), :]).astype(BF16).astype(F32)
        wide = h_ref[part(t), :].astype(F32)
        scale = lax.rsqrt(jnp.mean(wide * wide, -1, keepdims=True) + 1e-6)
        along = jnp.mean(by_a * wide, -1, keepdims=True)
        by_h = (by_a * scale - wide * (scale * scale * scale * along)).astype(BF16)
        return (DY[own_block(t), :].astype(F32) + by_h.astype(F32)).astype(BF16)

    def chunk(c):
        l = 1 - c // 8
        j = lax.rem(c, 8)
        i, hh = turn(l, j // 2), lax.rem(j, 2)
        pair = c // 2
        base = ROUNDS * l + 3 * i
        up_slot, down_slot = term(3 * pair + hh), term(3 * pair + 2)

        lo = jnp.where(c == 8, BETWEEN[1], events_by(c))
        count = events_by(c + 1) - lo

        ag_lo, ag_count = pick(SECOND[:-1], c), pick((*SECOND[1:], LAST_AG), c) - pick(SECOND[:-1], c)

        def serve(slot):
            ag_events(ag_lo + (ag_count * slot) // 8, ag_lo + (ag_count * slot + ag_count) // 8)
            rs_events(lo + (count * slot + 2) // 8, lo + (count * slot + count + 2) // 8)

        @pl.when(c == 8)
        def _():
            start, end = BETWEEN
            again = pltpu.make_async_copy(x_ref, A.at[mine], loc.at[1])
            again.start()
            send_xp.wait_recv()
            other = pltpu.make_async_copy(xp_ref, A.at[theirs], loc.at[2])
            other.start()
            fetch = pltpu.make_async_copy(h1_ref, DG.at[pl.ds(0, tok)], loc.at[0])
            fetch.start()
            rs_events(start, start + 1)
            fetch.wait()
            swap(0).wait()
            swap(1).wait()

            def body(t):
                dh = norm_back(DG, t)
                DY[own_block(t), :] = dh
                ACT[part(t), :] = dh

            loop(tok // block, body)
            send = remote(ACT.at[pl.ds(0, tok)], DY.at[mine], ex_send.at[4], ex_recv.at[4], mate)
            send.start()
            clear()
            flip_dy(core)
            rs_events(start + 1, start + 2)
            again.wait()
            norm_block(core, True)
            rs_events(start + 2, start + 3)
            other.wait()
            norm_block(1 - core, True)
            rs_events(start + 3, end)
            send.wait()
            flip_dy(1 - core)

            def gone(g):
                ag_retire(g)

            loop(GATHERED, gone, GATHERED - S_SLOTS)
            across_sent(1)

        @pl.when(l == 1)
        def _():
            @pl.when(hh == 0)
            def _():
                ag_ready(base)

            ag_ready(base + 1 + hh)

        def tokens(t):
            s = nth(t)
            at = A[s, :]
            wg, wu = W[base + 1 + hh, :, 0].reshape(d, -1), W[base + 1 + hh, :, 1].reshape(d, -1)
            gate, up = nn(at, wg), nn(at, wu)
            by_act = nt(DY[s, :], W[base, pl.ds(4 * hh, 4)].reshape(-1, d)).astype(BF16).astype(F32)
            sig = 0.5 * jnp.tanh(0.5 * gate) + 0.5
            silu = gate * sig
            ACT[s, :] = (silu * up).astype(BF16)
            dup = (by_act * silu).astype(BF16)
            dgate = (by_act * up * (sig + silu * (1.0 - sig))).astype(BF16)
            DG[s, :] = dgate
            DU[s, :] = dup
            ACC[s, :] += nt(dgate, wg) + nt(dup, wu)

            @pl.when((j == 7) & (t < 2))
            def _():
                swap(t).start()

            serve(t)

        loop(4, tokens)

        for back, when in ((0, 0), (1, 1), (2, 0)):
            n = 3 * pair + back - T_SLOTS

            @pl.when((hh == when) & (n >= 0))
            def _():
                rs_retire(n)

        def grads_up(p):
            s = pl.ds(pl.multiple_of(p * (d // 2), d // 2), d // 2)
            W[up_slot, pl.ds(4 * p, 4), 0] = nn(AT[s, :], DG[...]).astype(BF16).reshape(4, half, -1)
            W[up_slot, pl.ds(4 * p, 4), 1] = nn(AT[s, :], DU[...]).astype(BF16).reshape(4, half, -1)
            serve(4 + p)

        loop(2, grads_up)

        for p in range(2):
            s = slice(p * (d // 2), (p + 1) * (d // 2))
            g = nn(DYT[s, :], ACT[...]).T.astype(BF16)
            W[down_slot, pl.ds(4 * hh, 4), :, :, s] = g.reshape(4, 2, half, d // 2)
            serve(6 + p)

    loop(16, chunk)

    fetch = pltpu.make_async_copy(x_ref, DG.at[pl.ds(0, tok)], loc.at[0])
    fetch.start()
    rs_events(110, 111)
    fetch.wait()
    swap(0).wait()
    swap(1).wait()

    def last(t):
        ACT[part(t), :] = norm_back(DG, t)

    loop(tok // block, last)
    put = pltpu.make_async_copy(ACT.at[pl.ds(0, tok)], dx_ref, loc.at[1])
    put.start()
    rs_retire(ALL - T_SLOTS)
    rs_events(111, LAST_RS, True)

    put.wait()
    for copy in (send_x, send_xp, send_dy):
        copy.wait_send()

    def sent(n):
        rs_retire(n)

    for n in (ALL - 1, ALL):
        rs_retire(jnp.int32(n), True)
    across_sent(0)
    loop(ALL - 1, sent, ALL - T_SLOTS + 1)
    ups = W.at[0]
    remote(ups, ups, out_send.at[0], out_recv, mate).wait_recv()


def put_kernel(dx_ref, og_ref, od_ref, dx_out, dwg_out, dwu_out, dwd_out, dx, og, od, dwg, dwu, came, went):
    layers, _, ff = dwg.shape
    strip = ff // 64

    def copies(pairs, sems):
        return [pltpu.make_async_copy(src, dst, sems.at[k]) for k, (src, dst) in enumerate(pairs)]

    each = range(layers)
    loads = copies([(dx_ref, dx), (od_ref, od)] + [(og_ref.at[l], og.at[l]) for l in each], came)
    stores = [(dx, dx_out), (od, dwd_out)]
    stores = copies(stores + [(a.at[l], b.at[l]) for l in each for a, b in ((dwg, dwg_out), (dwu, dwu_out))], went)
    first = loads[:layers], stores[:layers]
    for copy in loads:
        copy.start()
    for load, store in zip(*first, strict=True):
        load.wait()
        store.start()
    for l in each:
        loads[layers + l].wait()
        for part in range(16):
            c, i, hh = part // 8, part // 2 % 4, part % 2
            for s in range(4):
                column = strip * (8 * (4 * hh + s) + 4 * c + i)
                for g, out in enumerate((dwg, dwu)):
                    out[l, :, column : column + strip] = og[l, c, i, hh, g, :, strip * s : strip * (s + 1)]
        for store in stores[2 * (l + 1) : 2 * (l + 2)]:
            store.start()
    for store in stores:
        store.wait()


def of_a_device(x, dy, w_gate, w_up, w_down):
    _, tok, d = x.shape
    layers, rows, ff = w_gate.shape
    half = 2 * rows
    strip = ff // 64
    wd = w_down.reshape(layers, 4, 2, half, d)
    hbm = pl.BlockSpec(memory_space=pltpu.HBM)
    tile = tok // 2
    piece = (2, half, d)
    both = 2 * tok
    dma = pltpu.SemaphoreType.DMA
    up = (layers, 2, 4, 2, 2, rows, 4 * strip)
    dx, og, od, _, _ = pl.pallas_call(
        functools.partial(kernel, tile),
        out_shape=tuple(
            jax.ShapeDtypeStruct(shape, BF16)
            for shape in ((tok, d), up, wd.shape, (tok, d), (tok, d))
        ),
        in_specs=[hbm] * 5,
        out_specs=[hbm] * 5,
        scratch_shapes=[
            pltpu.VMEM((ALL + T_SLOTS, 8, *piece), BF16),
            pltpu.VMEM((7 * R_SLOTS, *piece), BF16),
            pltpu.VMEM((both, d), BF16),
            pltpu.VMEM((d, both), BF16),
            pltpu.VMEM((both, d), BF16),
            pltpu.VMEM((d, both), BF16),
            pltpu.VMEM((both, d), F32),
            pltpu.VMEM((tok, d), F32),
            pltpu.VMEM((both, 4 * strip), BF16),
            pltpu.VMEM((both, 4 * strip), BF16),
            pltpu.VMEM((both, 4 * strip), BF16),
            dma((ALL // 3,)),
            dma((layers,)),
            dma(()),
            dma((2 * ALL // 3,)),
            dma((S_SLOTS, 2)),
            dma((S_SLOTS, 2, 4)),
            dma((2,)),
            dma((10,)),
            dma((T_SLOTS, 2)),
            dma((R_SLOTS, 2, 4)),
            dma((T_SLOTS,)),
            dma((T_SLOTS,)),
            dma(()),
            dma((5,)),
            dma((5,)),
            dma((2,)),
            dma((2,)),
            dma((3,)),
            pltpu.SemaphoreType.REGULAR((2,)),
        ],
        compiler_params=pltpu.CompilerParams(
            collective_id=0, has_side_effects=True, vmem_limit_bytes=67043328
        ),
    )(x[0], dy[0], w_gate, w_up, wd)
    results = (dx.shape, w_gate.shape, w_up.shape, od.shape)
    dx, dwg, dwu, dwd = pl.pallas_call(
        put_kernel,
        out_shape=tuple(jax.ShapeDtypeStruct(shape, BF16) for shape in results),
        in_specs=[hbm] * 3,
        out_specs=[hbm] * 4,
        scratch_shapes=[
            *(pltpu.VMEM(shape, BF16) for shape in (dx.shape, up, od.shape, w_gate.shape, w_up.shape)),
            dma((4,)),
            dma((6,)),
        ],
    )(dx, og, od)
    return dx[None], dwg, dwu, dwd.reshape(w_down.shape)


def solution(mesh):
    by_seq, by_row = P(("rep", "dp"), None, None), P(None, "dp", None)
    out = P("rep", "dp", None)
    return jax.shard_map(
        of_a_device,
        mesh=mesh,
        in_specs=(by_seq, by_seq, by_row, by_row, by_row),
        out_specs=(by_seq, out, out, out),
        check_vma=False,
    )
```

```python
import functools

import jax
import jax.numpy as jnp
from jax import lax
from jax.experimental import pallas as pl
from jax.experimental.pallas import tpu as pltpu
from jax.sharding import PartitionSpec as P

MESH = pl.DeviceIdType.MESH
F32, BF16 = jnp.float32, jnp.bfloat16
ROUNDS = 12
ALL = 2 * ROUNDS
T_SLOTS, R_SLOTS, S_SLOTS = 8, 6, 6
GATHERED = 14
FIRST = (25, 28, 31, 37, 41, 47, 50, 52, 55)
BETWEEN = 45, 51
SECOND = (62, 67, 77, 82, 82)
LAST_AG, LAST_RS = 5 * (GATHERED - 1) + 17, 5 * ALL + 17


def events_by(c):
    return jnp.where(c <= 8, jnp.maximum((13 * c - 14) // 2, jnp.minimum(c, 1)), (15 * c - 19) // 2)


def pick(values, k):
    out = values[-1]
    for number, value in enumerate(values[:-1]):
        out = jnp.where(k == number, value, out)
    return out


def loop(end, body, start=0):
    def step(k, carry):
        body(k)
        return carry

    lax.fori_loop(start, end, step, 0)


def nn(a, b):
    return jnp.dot(a, b, preferred_element_type=F32)


def nt(a, b):
    return lax.dot_general(a, b, (((1,), (1,)), ((), ())), preferred_element_type=F32)


def kernel(tile, x_ref, dy_ref, wg_ref, wu_ref, wd_ref, dx_ref, og_ref, od_ref, xp_ref, h1_ref,
           W, R, A, AT, DY, DYT, ACC, PT, ACT, DG, DU,
           prep_loc, prep_up, prep_send, prep_rem, ag_send, ag_recv, ax_send, ax_recv,
           rs_send, rs_recv, out_loc, out_send, out_recv, ex_send, ex_recv, sw_send, sw_recv, loc, credit):
    tok, d = x_ref.shape
    half = wd_ref.shape[3]
    rows = half // 2
    strip = wg_ref.shape[2] // 64
    assert d == 4 * strip and half == strip // 2
    rep, dp = lax.axis_index("rep"), lax.axis_index("dp")
    core, chip = lax.rem(dp, 2), dp // 2
    q = jnp.where(chip < 4, chip, 11 - chip)

    def chip_at(place):
        place = lax.rem(place + 16, 8)
        return jnp.where(place < 4, place, 11 - place)

    ring = tuple((rep, 2 * chip_at(q + step) + core) for step in (1, -1))
    across, mate = (1 - rep, dp), (rep, 2 * chip + 1 - core)

    def remote(src, dst, send, recv, to):
        return pltpu.make_async_remote_copy(
            src_ref=src, dst_ref=dst, send_sem=send, recv_sem=recv, device_id=to, device_id_type=MESH
        )

    barrier = pltpu.get_barrier_semaphore()
    for other in (*ring, across, mate):
        pl.semaphore_signal(barrier, inc=1, device_id=other, device_id_type=MESH)

    mine, theirs = pl.ds(core * tok, tok), pl.ds((1 - core) * tok, tok)
    own_rows = pl.ds(pl.multiple_of(core * rows, rows), rows)
    mate_rows = pl.ds(pl.multiple_of((1 - core) * rows, rows), rows)

    def kind(r):
        return lax.rem(r, 3)

    def prep_down(r):
        src = wd_ref.at[r // ROUNDS, lax.rem(r, ROUNDS) // 3]
        return pltpu.make_async_copy(src, W.at[r, chip], prep_loc.at[r // 3])

    def staged(l, g, b, columns=slice(None)):
        spot = 16 * g + b
        return 8 * l + spot // 4, lax.rem(spot // 2, 2), pl.ds(pl.multiple_of(rows * lax.rem(spot, 2), rows), rows), columns

    def load_up(l):
        def body(b):
            for g, ref in enumerate((wg_ref, wu_ref)):
                src = ref.at[l, :, pl.ds(pl.multiple_of(d * b, d), d)]
                pltpu.make_async_copy(src, R.at[staged(l, g, b)], prep_up.at[l]).start()

        loop(16, body)

    def loaded_up(l):
        eight = R.at[pl.ds(8 * l, 8)]
        pltpu.make_async_copy(eight, eight, prep_up.at[l]).wait()

    def up_number(r):
        return 2 * (r // 3) + kind(r) - 1

    def mate_part(r, g):
        return pl.ds(pl.multiple_of((2 * up_number(r) + g) * rows, rows), rows)

    def prep_start(r):
        l, i, hh = r // ROUNDS, lax.rem(r, ROUNDS) // 3, kind(r) - 1
        columns = pl.ds(pl.multiple_of(strip * i, strip), strip)
        for g in range(2):
            for s in range(4):
                place = slice(strip * s, strip * (s + 1))
                b = 2 * (4 * hh + s)
                W[r, chip, g, own_rows, place] = R[staged(l, g, b + core, columns)]
                DG[mate_part(r, g), place] = R[staged(l, g, b + 1 - core, columns)]
            dst = W.at[r, chip, g, own_rows]
            remote(DG.at[mate_part(r, g)], dst, prep_send, prep_rem.at[up_number(r)], mate).start()

    def prep_there(r):
        part = W.at[r, chip, :, own_rows]
        return remote(part, part, prep_send, prep_rem.at[up_number(r)], mate)

    def prep_first(r):
        prep_down(3 * r).start()

    load_up(0)
    loop(ALL // 3, prep_first)
    load_up(1)

    def prep_all(lo, hi):
        def body(r):
            @pl.when(kind(r) != 0)
            def _():
                prep_start(r)

        loop(hi, body, lo)

    load_x = pltpu.make_async_copy(x_ref, A.at[mine], loc.at[0])
    load_dy = pltpu.make_async_copy(dy_ref, DY.at[mine], loc.at[1])
    load_x.start()
    load_dy.start()
    pl.semaphore_wait(barrier, 4)

    send_x = remote(x_ref, A.at[mine], ex_send.at[0], ex_recv.at[0], mate)
    send_xp = remote(x_ref, xp_ref, ex_send.at[1], ex_recv.at[1], mate)
    send_dy = remote(dy_ref, DY.at[mine], ex_send.at[2], ex_recv.at[2], mate)
    loaded_up(0)
    prep_all(0, 3)
    send_x.start()
    send_xp.start()
    send_dy.start()

    def wait_prep(r):
        @pl.when(lax.rem(r, 3) == 0)
        def _():
            prep_down(r).wait()

        @pl.when(lax.rem(r, 3) != 0)
        def _():
            prep_there(r).wait_recv()

    def hops(r, way):
        return 4 - lax.rem(r + way + 8, 2)

    def shared(r):
        return (r >= ROUNDS) | (kind(r) != 2)

    def gathers(r):
        first = (kind(r) == 2) | (kind(r) == rep)
        return jnp.where(r < ROUNDS, first, (r - ROUNDS) // 6 == rep)

    def across_number(r):
        return jnp.where(r < ROUNDS, r // 3, 4 + lax.rem(r, 6))

    def gathered(g):
        return jnp.where(
            g < 8, pick((rep, 3 + rep, 2, 6 + rep, 5, 9 + rep, 8, 11), g), ROUNDS + 6 * rep + g - 8
        )

    def ag_copy(g, r, way, h):
        piece = W.at[r, chip_at(q - h if way == 0 else q + h)]
        slot = lax.rem(g, S_SLOTS)
        return remote(piece, piece, ag_send.at[slot, way], ag_recv.at[slot, way, h], ring[way])

    def ag_retire(g):
        for way in (0, 1):
            for count in (3, 4):
                @pl.when(hops(g, way) == count)
                def _():
                    sent = W.at[0, pl.ds(0, count)]
                    remote(sent, sent, ag_send.at[lax.rem(g, S_SLOTS), way], ag_recv.at[0, way, 0], ring[way]).wait_send()

    def ag_event(g, h):
        @pl.when((g >= 0) & (g < GATHERED))
        def _():
            r = gathered(g)

            @pl.when(h == 0)
            def _():
                wait_prep(r)

                @pl.when(g >= S_SLOTS)
                def _():
                    ag_retire(g - S_SLOTS)

            for way in (0, 1):
                @pl.when(h == 0)
                def _():
                    ag_copy(g, r, way, 0).start()

                @pl.when((h > 0) & (h <= hops(g, way)))
                def _():
                    ag_copy(g, r, way, h - 1).wait_recv()

                    @pl.when(h < hops(g, way))
                    def _():
                        ag_copy(g, r, way, h).start()

                    @pl.when(shared(r))
                    def _():
                        piece = W.at[r, chip_at(q - h if way == 0 else q + h)]
                        remote(piece, piece, ax_send.at[r // ROUNDS], ax_recv.at[across_number(r)], across).start()

    def ag_ready(r):
        @pl.when(jnp.logical_not(gathers(r)))
        def _():
            wait_prep(r)
            seven = W.at[r, pl.ds(0, 7)]
            remote(seven, seven, ax_send.at[0], ax_recv.at[across_number(r)], across).wait_recv()

    def across_sent(l):
        some = W.at[pl.ds(0, 7), pl.ds(0, 4)] if l == 0 else W.at[pl.ds(0, 7), pl.ds(0, 6)]
        remote(some, some, ax_send.at[l], ax_recv.at[0], across).wait_send()

    def ag_events(lo, hi):
        def body(e):
            h = lax.rem(4 * e, 5)
            ag_event((e - 4 * h) // 5, h)

        loop(hi, body, lo)

    def turn(l, k):
        return jnp.where(l == 1, lax.rem(k + 2 * rep, 4), k)

    def strip_of(n):
        return turn(1 - n // ROUNDS, lax.rem(n, ROUNDS) // 3)

    def term(n):
        return jnp.where(n < ROUNDS, ALL + lax.rem(n, T_SLOTS), n)

    def own_sem(n):
        return lax.rem(n, T_SLOTS)

    def spot(n, owner, cut):
        return (ALL - 1, owner, n - (ALL - 1)) if cut else (term(n), owner)

    def came(n, way, h, cut):
        place = 7 * lax.rem(n, R_SLOTS) + (h if way == 0 else hops(n, 0) + h)
        return (place, 0) if cut else (place,)

    def rs_copy(n, way, h, cut):
        step = hops(n, way) - h
        return remote(
            W.at[spot(n, chip_at(q + step if way == 0 else q - step), cut)],
            R.at[came(n, way, h, cut)],
            rs_send.at[own_sem(n), way],
            rs_recv.at[lax.rem(n, R_SLOTS), way, h],
            ring[way],
        )

    def out_down(n, cut):
        dst = (0, 3, n - (ALL - 1)) if cut else (1 - n // ROUNDS, strip_of(n))
        return pltpu.make_async_copy(W.at[spot(n, chip, cut)], od_ref.at[dst], out_loc.at[own_sem(n)])

    def out_up(n):
        return og_ref.at[1 - n // ROUNDS, core, strip_of(n), jnp.minimum(kind(n), 1)]

    def out_here(n):
        return pltpu.make_async_copy(W.at[term(n), chip, :, own_rows], out_up(n), out_loc.at[own_sem(n)])

    def out_there(n):
        part = W.at[term(n), chip, :, mate_rows]
        return remote(part, out_up(n), out_send.at[own_sem(n)], out_recv, mate)

    def rs_retire(n, cut=False):
        for way in (0, 1):
            for count in (3, 4):
                @pl.when(hops(n, way) == count)
                def _():
                    sent = W.at[spot(n, pl.ds(0, count), cut)]
                    remote(sent, sent, rs_send.at[own_sem(n), way], rs_recv.at[0, way, 0], ring[way]).wait_send()

        if cut:
            out_down(n, cut).wait()
            return

        @pl.when(kind(n) == 2)
        def _():
            out_down(n, cut).wait()

        @pl.when(kind(n) != 2)
        def _():
            out_here(n).wait()
            out_there(n).wait_send()

    def rs_event(n, h, cut):
        for way in (0, 1):
            @pl.when(h == 0)
            def _():
                @pl.when(n >= R_SLOTS)
                def _():
                    pl.semaphore_wait(credit.at[way], 1)

                rs_copy(n, way, 0, cut).start()

            @pl.when((h > 0) & (h <= hops(n, way)))
            def _():
                rs_copy(n, way, h - 1, cut).wait_recv()

                @pl.when(h < hops(n, way))
                def _():
                    step = hops(n, way) - h
                    own = spot(n, chip_at(q + step if way == 0 else q - step), cut)
                    total = W[own].astype(F32) + R[came(n, way, h - 1, cut)].astype(F32)
                    W[own] = total.astype(BF16)
                    rs_copy(n, way, h, cut).start()

        @pl.when(h == 4)
        def _():
            own = spot(n, chip, cut)
            total = W[own].astype(F32) + R[came(n, 0, hops(n, 0) - 1, cut)].astype(F32)
            total = total + R[came(n, 1, hops(n, 1) - 1, cut)].astype(F32)
            W[own] = total.astype(BF16)
            if cut:
                out_down(n, cut).start()
                return

            @pl.when(kind(n) == 2)
            def _():
                out_down(n, cut).start()

            @pl.when(kind(n) != 2)
            def _():
                out_here(n).start()
                out_there(n).start()

            @pl.when(n <= ALL - R_SLOTS)
            def _():
                for way in (0, 1):
                    pl.semaphore_signal(credit.at[way], inc=1, device_id=ring[1 - way], device_id_type=MESH)

    def rs_events(lo, hi, end=False):
        def body(e):
            h = lax.rem(4 * e, 5)
            n = (e - 4 * h) // 5

            @pl.when((n >= 0) & (n < ALL - 1))
            def _():
                rs_event(n, h, False)

            if end:
                @pl.when((n >= ALL - 1) & (n <= ALL))
                def _():
                    rs_event(n, h, True)

        loop(hi, body, lo)

    block = min(256, tok)
    blocks = 2 * tok // block

    def part(t, size=block):
        return pl.ds(pl.multiple_of(t * size, size), size)

    def normed(h):
        wide = h.astype(F32)
        return (wide * lax.rsqrt(jnp.mean(wide * wide, -1, keepdims=True) + 1e-6)).astype(BF16)

    def block_of(c, t):
        return pl.ds(pl.multiple_of(c * tok + t * block, block), block)

    def norm_block(c, flip):
        def body(t):
            s = block_of(c, t)
            a = normed(A[s, :])
            A[s, :] = a
            if flip:
                AT[:, s] = a.T

        loop(tok // block, body)

    def flip_dy(c):
        def body(t):
            s = block_of(c, t)
            DYT[:, s] = DY[s, :].T

        loop(tok // block, body)

    def clear():
        def body(t):
            ACC[part(t), :] = jnp.zeros((block, d), F32)

        loop(blocks, body)

    def own_block(t):
        return block_of(core, t)

    def nth(t):
        return part(lax.rem(t + 2 * (1 - core), 4), tile)

    def swap(t):
        src = ACC.at[pl.ds(pl.multiple_of((1 - core) * tok + t * tile, tile), tile)]
        return remote(src, PT.at[part(t, tile)], sw_send.at[t], sw_recv.at[t], mate)

    def forward(j, after):
        i, hh = j // 2, lax.rem(j, 2)
        r = 3 * i + 1 + hh

        def body(t):
            s = nth(t)
            at = A[s, :]
            gate = nn(at, W[r, :, 0].reshape(d, -1))
            up = nn(at, W[r, :, 1].reshape(d, -1))
            act = (gate * (0.5 * jnp.tanh(0.5 * gate) + 0.5) * up).astype(BF16)
            ACC[s, :] += nn(act, W[3 * i, pl.ds(4 * hh, 4)].reshape(-1, d))

            @pl.when((j == 7) & (t < 2))
            def _():
                swap(t).start()

            after(t)

        loop(4, body)

    ag_events(0, 1)
    prep_all(3, ROUNDS)
    ag_events(1, 4)
    loaded_up(1)
    prep_all(ROUNDS, ALL)
    load_x.wait()
    norm_block(core, False)
    ag_events(4, 6)
    send_x.wait_recv()
    norm_block(1 - core, False)
    clear()
    ag_events(6, 9)
    load_dy.wait()
    flip_dy(core)
    ag_events(9, 11)
    send_dy.wait_recv()
    flip_dy(1 - core)
    ag_events(11, FIRST[0])

    def first(j):
        i, hh = j // 2, lax.rem(j, 2)

        @pl.when(hh == 0)
        def _():
            ag_ready(3 * i)

        ag_ready(3 * i + 1 + hh)
        lo, count = pick(FIRST[:8], j), pick(FIRST[1:], j) - pick(FIRST[:8], j)
        forward(j, lambda t: ag_events(lo + (count * t) // 4, lo + (count * (t + 1)) // 4))

    loop(8, first)

    whole = DG.at[pl.ds(0, 4 * ALL // 3 * rows)]
    remote(whole, whole, prep_send, prep_rem.at[0], mate).wait_send()
    fetch = pltpu.make_async_copy(x_ref, DG.at[pl.ds(0, tok)], loc.at[0])
    fetch.start()
    ag_events(55, 57)
    fetch.wait()
    swap(0).wait()
    swap(1).wait()

    def residual(t):
        mlp = (ACC[own_block(t), :] + PT[part(t), :]).astype(BF16)
        h = (DG[part(t), :].astype(F32) + mlp.astype(F32)).astype(BF16)
        ACT[part(t), :] = h
        A[own_block(t), :] = h

    loop(tok // block, residual)
    h1 = ACT.at[pl.ds(0, tok)]
    send_h = remote(h1, A.at[mine], ex_send.at[3], ex_recv.at[3], mate)
    keep_h = pltpu.make_async_copy(h1, h1_ref, loc.at[1])
    send_h.start()
    keep_h.start()
    clear()
    norm_block(core, True)
    ag_events(57, 60)
    send_h.wait()
    norm_block(1 - core, True)
    ag_events(60, 62)
    keep_h.wait()

    def norm_back(h_ref, t):
        by_a = (ACC[own_block(t), :] + PT[part(t), :]).astype(BF16).astype(F32)
        wide = h_ref[part(t), :].astype(F32)
        scale = lax.rsqrt(jnp.mean(wide * wide, -1, keepdims=True) + 1e-6)
        along = jnp.mean(by_a * wide, -1, keepdims=True)
        by_h = (by_a * scale - wide * (scale * scale * scale * along)).astype(BF16)
        return (DY[own_block(t), :].astype(F32) + by_h.astype(F32)).astype(BF16)

    def chunk(c):
        l = 1 - c // 8
        j = lax.rem(c, 8)
        i, hh = turn(l, j // 2), lax.rem(j, 2)
        pair = c // 2
        base = ROUNDS * l + 3 * i
        up_slot, down_slot = term(3 * pair + hh), term(3 * pair + 2)

        lo = jnp.where(c == 8, BETWEEN[1], events_by(c))
        count = events_by(c + 1) - lo

        ag_lo, ag_count = pick(SECOND[:-1], c), pick((*SECOND[1:], LAST_AG), c) - pick(SECOND[:-1], c)

        def serve(slot):
            ag_events(ag_lo + (ag_count * slot) // 8, ag_lo + (ag_count * slot + ag_count) // 8)
            rs_events(lo + (count * slot + 2) // 8, lo + (count * slot + count + 2) // 8)

        @pl.when(c == 8)
        def _():
            start, end = BETWEEN
            again = pltpu.make_async_copy(x_ref, A.at[mine], loc.at[1])
            again.start()
            send_xp.wait_recv()
            other = pltpu.make_async_copy(xp_ref, A.at[theirs], loc.at[2])
            other.start()
            fetch = pltpu.make_async_copy(h1_ref, DG.at[pl.ds(0, tok)], loc.at[0])
            fetch.start()
            rs_events(start, start + 1)
            fetch.wait()
            swap(0).wait()
            swap(1).wait()

            def body(t):
                dh = norm_back(DG, t)
                DY[own_block(t), :] = dh
                ACT[part(t), :] = dh

            loop(tok // block, body)
            send = remote(ACT.at[pl.ds(0, tok)], DY.at[mine], ex_send.at[4], ex_recv.at[4], mate)
            send.start()
            clear()
            flip_dy(core)
            rs_events(start + 1, start + 2)
            again.wait()
            norm_block(core, True)
            rs_events(start + 2, start + 3)
            other.wait()
            norm_block(1 - core, True)
            rs_events(start + 3, end)
            send.wait()
            flip_dy(1 - core)

            def gone(g):
                ag_retire(g)

            loop(GATHERED, gone, GATHERED - S_SLOTS)
            across_sent(1)

        @pl.when(l == 1)
        def _():
            @pl.when(hh == 0)
            def _():
                ag_ready(base)

            ag_ready(base + 1 + hh)

        def tokens(t):
            s = nth(t)
            at = A[s, :]
            wg, wu = W[base + 1 + hh, :, 0].reshape(d, -1), W[base + 1 + hh, :, 1].reshape(d, -1)
            gate, up = nn(at, wg), nn(at, wu)
            by_act = nt(DY[s, :], W[base, pl.ds(4 * hh, 4)].reshape(-1, d)).astype(BF16).astype(F32)
            sig = 0.5 * jnp.tanh(0.5 * gate) + 0.5
            silu = gate * sig
            ACT[s, :] = (silu * up).astype(BF16)
            dup = (by_act * silu).astype(BF16)
            dgate = (by_act * up * (sig + silu * (1.0 - sig))).astype(BF16)
            DG[s, :] = dgate
            DU[s, :] = dup
            ACC[s, :] += nt(dgate, wg) + nt(dup, wu)

            @pl.when((j == 7) & (t < 2))
            def _():
                swap(t).start()

            serve(t)

        loop(4, tokens)

        for back, when in ((0, 0), (1, 1), (2, 0)):
            n = 3 * pair + back - T_SLOTS

            @pl.when((hh == when) & (n >= 0))
            def _():
                rs_retire(n)

        def grads_up(p):
            s = pl.ds(pl.multiple_of(p * (d // 2), d // 2), d // 2)
            W[up_slot, pl.ds(4 * p, 4), 0] = nn(AT[s, :], DG[...]).astype(BF16).reshape(4, half, -1)
            W[up_slot, pl.ds(4 * p, 4), 1] = nn(AT[s, :], DU[...]).astype(BF16).reshape(4, half, -1)
            serve(4 + p)

        loop(2, grads_up)

        for p in range(2):
            s = slice(p * (d // 2), (p + 1) * (d // 2))
            g = nn(DYT[s, :], ACT[...]).T.astype(BF16)
            W[down_slot, pl.ds(4 * hh, 4), :, :, s] = g.reshape(4, 2, half, d // 2)
            serve(6 + p)

    loop(16, chunk)

    fetch = pltpu.make_async_copy(x_ref, DG.at[pl.ds(0, tok)], loc.at[0])
    fetch.start()
    rs_events(110, 111)
    fetch.wait()
    swap(0).wait()
    swap(1).wait()

    def last(t):
        ACT[part(t), :] = norm_back(DG, t)

    loop(tok // block, last)
    put = pltpu.make_async_copy(ACT.at[pl.ds(0, tok)], dx_ref, loc.at[1])
    put.start()
    rs_retire(ALL - T_SLOTS)
    rs_events(111, LAST_RS, True)

    put.wait()
    for copy in (send_x, send_xp, send_dy):
        copy.wait_send()

    def sent(n):
        rs_retire(n)

    for n in (ALL - 1, ALL):
        rs_retire(jnp.int32(n), True)
    across_sent(0)
    loop(ALL - 1, sent, ALL - T_SLOTS + 1)
    ups = W.at[0]
    remote(ups, ups, out_send.at[0], out_recv, mate).wait_recv()


def put_kernel(dx_ref, og_ref, od_ref, dx_out, dwg_out, dwu_out, dwd_out, dx, og, od, dwg, dwu, came, went):
    layers, _, ff = dwg.shape
    strip = ff // 64

    def copies(pairs, sems):
        return [pltpu.make_async_copy(src, dst, sems.at[k]) for k, (src, dst) in enumerate(pairs)]

    each = range(layers)
    loads = copies([(dx_ref, dx), (od_ref, od)] + [(og_ref.at[l], og.at[l]) for l in each], came)
    stores = [(dx, dx_out), (od, dwd_out)]
    stores = copies(stores + [(a.at[l], b.at[l]) for l in each for a, b in ((dwg, dwg_out), (dwu, dwu_out))], went)
    first = loads[:layers], stores[:layers]
    for copy in loads:
        copy.start()
    for load, store in zip(*first, strict=True):
        load.wait()
        store.start()
    for l in each:
        loads[layers + l].wait()
        for part in range(16):
            c, i, hh = part // 8, part // 2 % 4, part % 2
            for s in range(4):
                column = strip * (8 * (4 * hh + s) + 4 * c + i)
                for g, out in enumerate((dwg, dwu)):
                    out[l, :, column : column + strip] = og[l, c, i, hh, g, :, strip * s : strip * (s + 1)]
        for store in stores[2 * (l + 1) : 2 * (l + 2)]:
            store.start()
    for store in stores:
        store.wait()


def of_a_device(x, dy, w_gate, w_up, w_down):
    _, tok, d = x.shape
    layers, rows, ff = w_gate.shape
    half = 2 * rows
    strip = ff // 64
    wd = w_down.reshape(layers, 4, 2, half, d)
    hbm = pl.BlockSpec(memory_space=pltpu.HBM)
    tile = tok // 2
    piece = (2, half, d)
    both = 2 * tok
    dma = pltpu.SemaphoreType.DMA
    up = (layers, 2, 4, 2, 2, rows, 4 * strip)
    dx, og, od, _, _ = pl.pallas_call(
        functools.partial(kernel, tile),
        out_shape=tuple(
            jax.ShapeDtypeStruct(shape, BF16)
            for shape in ((tok, d), up, wd.shape, (tok, d), (tok, d))
        ),
        in_specs=[hbm] * 5,
        out_specs=[hbm] * 5,
        scratch_shapes=[
            pltpu.VMEM((ALL + T_SLOTS, 8, *piece), BF16),
            pltpu.VMEM((7 * R_SLOTS, *piece), BF16),
            pltpu.VMEM((both, d), BF16),
            pltpu.VMEM((d, both), BF16),
            pltpu.VMEM((both, d), BF16),
            pltpu.VMEM((d, both), BF16),
            pltpu.VMEM((both, d), F32),
            pltpu.VMEM((tok, d), F32),
            pltpu.VMEM((both, 4 * strip), BF16),
            pltpu.VMEM((both, 4 * strip), BF16),
            pltpu.VMEM((both, 4 * strip), BF16),
            dma((ALL // 3,)),
            dma((layers,)),
            dma(()),
            dma((2 * ALL // 3,)),
            dma((S_SLOTS, 2)),
            dma((S_SLOTS, 2, 4)),
            dma((2,)),
            dma((10,)),
            dma((T_SLOTS, 2)),
            dma((R_SLOTS, 2, 4)),
            dma((T_SLOTS,)),
            dma((T_SLOTS,)),
            dma(()),
            dma((5,)),
            dma((5,)),
            dma((2,)),
            dma((2,)),
            dma((3,)),
            pltpu.SemaphoreType.REGULAR((2,)),
        ],
        compiler_params=pltpu.CompilerParams(
            collective_id=0, has_side_effects=True, vmem_limit_bytes=67043328
        ),
    )(x[0], dy[0], w_gate, w_up, wd)
    results = (dx.shape, w_gate.shape, w_up.shape, od.shape)
    dx, dwg, dwu, dwd = pl.pallas_call(
        put_kernel,
        out_shape=tuple(jax.ShapeDtypeStruct(shape, BF16) for shape in results),
        in_specs=[hbm] * 3,
        out_specs=[hbm] * 4,
        scratch_shapes=[
            *(pltpu.VMEM(shape, BF16) for shape in (dx.shape, up, od.shape, w_gate.shape, w_up.shape)),
            dma((4,)),
            dma((6,)),
        ],
    )(dx, og, od)
    return dx[None], dwg, dwu, dwd.reshape(w_down.shape)


def solution(mesh):
    by_seq, by_row = P(("rep", "dp"), None, None), P(None, "dp", None)
    out = P("rep", "dp", None)
    return jax.shard_map(
        of_a_device,
        mesh=mesh,
        in_specs=(by_seq, by_seq, by_row, by_row, by_row),
        out_specs=(by_seq, out, out, out),
        check_vma=False,
    )
```
